32 devices in a mesh: dp: 1 (over z), tp: 4 (over y), fsdp: 4 (over x), cp: 2 (over core).
Axes of the slice: x: 4, y: 4, z: 1, core: 2. Of those that a mesh axis runs over, the one named last changes fastest.
The devices are a block of a 4x4x8 slice.
Arguments:
- hidden: bfloat16 [4, 3072, 5120], P(('dp', 'fsdp'), 'cp')
- positions: int32 [4, 3072], P(('dp', 'fsdp'), 'cp')
- attn_gain: float32 [5120], replicated
- w_query: bfloat16 [5120, 32, 128], P(('fsdp', 'cp'), 'tp')
- w_key: bfloat16 [5120, 8, 128], P(('fsdp', 'cp'), 'tp')
- w_value: bfloat16 [5120, 8, 128], P(('fsdp', 'cp'), 'tp')
- w_out: bfloat16 [32, 128, 5120], P('tp', None, ('fsdp', 'cp'))
- mlp_gain: float32 [5120], replicated
- w_gate: bfloat16 [5120, 14336], P(('fsdp', 'cp'), 'tp')
- w_up: bfloat16 [5120, 14336], P(('fsdp', 'cp'), 'tp')
- w_down: bfloat16 [14336, 5120], P('tp', ('fsdp', 'cp'))
Outputs:
- output: bfloat16 [4, 3072, 5120], P(('dp', 'fsdp'), 'cp')
All inputs are finite; a program needn't handle non-finite values.
Results may differ from the reference program's by a relative error of at most 0.0134593.
Values are sent between devices in bfloat16 or wider.
A program may use at most 768 MiB of HBM per device.

```python
import numpy as np
import jax
import jax.numpy as jnp
from jax import lax

SEQS = 1
SEG_LEN = 768
CP = 2
FSDP = 4
D = 5120
HEADS = 32
KV_HEADS = 8
HEAD = 128
FF = 14336
QBLOCK = 128
ROPE_THETA = 500000.0
NORM_EPS = 1e-5
BATCH = FSDP * SEQS
SEQ = 2 * CP * SEG_LEN
GROUP = HEADS // KV_HEADS


def setup_inputs(seed: int = 0, part: int = 0) -> dict:
    part_keys = jax.random.split(jax.random.fold_in(jax.random.key(seed), part), 3)
    weight_keys = jax.random.split(jax.random.key(seed + 7919), 9)
    noise = jax.random.normal(part_keys[0], (BATCH, 2 * CP, SEG_LEN, D), jnp.float32)
    seg_mean = jax.random.normal(part_keys[1], (BATCH, 2 * CP, 1, D), jnp.float32)
    hidden = (0.6 * noise + seg_mean).reshape(BATCH, SEQ, D).astype(jnp.bfloat16)
    gaps = jax.random.randint(part_keys[2], (BATCH, SEQ), 1, 5, dtype=jnp.int32)
    true_pos = jnp.cumsum(gaps, axis=1) - 1
    seg_order = np.array([slot // 2 if slot % 2 == 0 else 2 * CP - 1 - slot // 2 for slot in range(2 * CP)])
    positions = true_pos.reshape(BATCH, 2 * CP, SEG_LEN)[:, seg_order].reshape(BATCH, SEQ).astype(jnp.int32)
    in_scale = D ** -0.5
    return {
        'hidden': hidden,
        'positions': positions,
        'attn_gain': 1.0 + 0.25 * jax.random.normal(weight_keys[0], (D,), jnp.float32),
        'w_query': (1.5 * in_scale * jax.random.normal(weight_keys[1], (D, HEADS, HEAD), jnp.float32)).astype(jnp.bfloat16),
        'w_key': (1.5 * in_scale * jax.random.normal(weight_keys[2], (D, KV_HEADS, HEAD), jnp.float32)).astype(jnp.bfloat16),
        'w_value': (in_scale * jax.random.normal(weight_keys[3], (D, KV_HEADS, HEAD), jnp.float32)).astype(jnp.bfloat16),
        'w_out': ((HEADS * HEAD) ** -0.5 * jax.random.normal(weight_keys[4], (HEADS, HEAD, D), jnp.float32)).astype(jnp.bfloat16),
        'mlp_gain': 1.0 + 0.25 * jax.random.normal(weight_keys[5], (D,), jnp.float32),
        'w_gate': (in_scale * jax.random.normal(weight_keys[6], (D, FF), jnp.float32)).astype(jnp.bfloat16),
        'w_up': (in_scale * jax.random.normal(weight_keys[7], (D, FF), jnp.float32)).astype(jnp.bfloat16),
        'w_down': (FF ** -0.5 * jax.random.normal(weight_keys[8], (FF, D), jnp.float32)).astype(jnp.bfloat16),
    }


def rms_norm(hidden_f32, gain):
    mean_sq = jnp.mean(hidden_f32 * hidden_f32, axis=-1, keepdims=True)
    return (hidden_f32 * lax.rsqrt(mean_sq + NORM_EPS) * gain).astype(jnp.bfloat16)


def rope_tables(positions):
    inv_freq = ROPE_THETA ** (-jnp.arange(0, HEAD, 2, dtype=jnp.float32) / HEAD)
    angles = positions.astype(jnp.float32)[..., None] * inv_freq
    return jnp.cos(angles)[..., None, :], jnp.sin(angles)[..., None, :]


def apply_rope(projected, rope_cos, rope_sin):
    half_dim = projected.shape[-1] // 2
    first_half = projected[..., :half_dim]
    second_half = projected[..., half_dim:]
    return jnp.concatenate([first_half * rope_cos - second_half * rope_sin, second_half * rope_cos + first_half * rope_sin], axis=-1)


def attention(queries, keys, values, positions):
    n_blocks = SEQ // QBLOCK
    q_blocks = queries.reshape(BATCH * n_blocks, QBLOCK, KV_HEADS, GROUP, HEAD)
    pos_blocks = positions.reshape(BATCH * n_blocks, QBLOCK)
    seq_ids = jnp.arange(BATCH * n_blocks) // n_blocks
    keys_f32 = keys.astype(jnp.float32)
    values_f32 = values.astype(jnp.float32)

    def one_block(block_args):
        q_blk, qpos_blk, seq_id = block_args
        k_seq = lax.dynamic_index_in_dim(keys_f32, seq_id, 0, keepdims=False)
        v_seq = lax.dynamic_index_in_dim(values_f32, seq_id, 0, keepdims=False)
        kpos_seq = lax.dynamic_index_in_dim(positions, seq_id, 0, keepdims=False)
        scores = jnp.einsum('qkgd,skd->kgqs', q_blk.astype(jnp.float32), k_seq) * (HEAD ** -0.5)
        visible = qpos_blk[:, None] >= kpos_seq[None, :]
        scores = jnp.where(visible, scores, -jnp.inf)
        row_max = jnp.max(scores, axis=-1, keepdims=True)
        probs = jnp.exp(scores - row_max)
        row_sum = jnp.sum(probs, axis=-1)
        weighted = jnp.einsum('kgqs,skd->qkgd', probs.astype(jnp.bfloat16).astype(jnp.float32), v_seq)
        return (weighted / jnp.transpose(row_sum, (2, 0, 1))[..., None]).astype(jnp.bfloat16)

    mixed = lax.map(one_block, (q_blocks, pos_blocks, seq_ids))
    return mixed.reshape(BATCH, SEQ, HEADS, HEAD)


def reference(hidden, positions, attn_gain, w_query, w_key, w_value, w_out, mlp_gain, w_gate, w_up, w_down):
    hidden_f32 = hidden.astype(jnp.float32)
    normed = rms_norm(hidden_f32, attn_gain).astype(jnp.float32)
    rope_cos, rope_sin = rope_tables(positions)
    queries = apply_rope(jnp.einsum('bsd,dhe->bshe', normed, w_query.astype(jnp.float32)), rope_cos, rope_sin).astype(jnp.bfloat16)
    keys = apply_rope(jnp.einsum('bsd,dhe->bshe', normed, w_key.astype(jnp.float32)), rope_cos, rope_sin).astype(jnp.bfloat16)
    values = jnp.einsum('bsd,dhe->bshe', normed, w_value.astype(jnp.float32)).astype(jnp.bfloat16)
    mixed = attention(queries.reshape(BATCH, SEQ, KV_HEADS, GROUP, HEAD), keys, values, positions)
    attn_out = jnp.einsum('bshe,hed->bsd', mixed.astype(jnp.float32), w_out.astype(jnp.float32)).astype(jnp.bfloat16)
    mid_resid = (hidden_f32 + attn_out.astype(jnp.float32)).astype(jnp.bfloat16)
    mid_f32 = mid_resid.astype(jnp.float32)
    normed_mlp = rms_norm(mid_f32, mlp_gain).astype(jnp.float32)
    gate_proj = jnp.einsum('bsd,df->bsf', normed_mlp, w_gate.astype(jnp.float32))
    up_proj = jnp.einsum('bsd,df->bsf', normed_mlp, w_up.astype(jnp.float32))
    act_mlp = (jax.nn.silu(gate_proj) * up_proj).astype(jnp.bfloat16)
    down_proj = jnp.einsum('bsf,fd->bsd', act_mlp.astype(jnp.float32), w_down.astype(jnp.float32)).astype(jnp.bfloat16)
    return (mid_f32 + down_proj.astype(jnp.float32)).astype(jnp.bfloat16)
```

```python
import functools

import jax
import jax.numpy as jnp
from jax import lax
from jax.experimental import pallas as pl
from jax.experimental.pallas import tpu as pltpu
from jax.sharding import PartitionSpec as P

ROPE_THETA = 500000.0
NORM_EPS = 1e-5
GROUP_AXES = ('fsdp', 'cp')
N_SUB = 4
F32 = jnp.float32
BF16 = jnp.bfloat16
MESH = pl.DeviceIdType.MESH
VMEM_BIG = 58 * 1024 * 1024
ANY = pl.BlockSpec(memory_space=pl.ANY)


def rms_norm(hidden_f32, gain):
    mean_sq = jnp.mean(hidden_f32 * hidden_f32, axis=-1, keepdims=True)
    return (hidden_f32 * lax.rsqrt(mean_sq + NORM_EPS) * gain).astype(BF16)


def rope_tables(positions, head_dim):
    inv_freq = ROPE_THETA ** (-jnp.arange(0, head_dim, 2, dtype=F32) / head_dim)
    angles = positions.astype(F32)[..., None] * inv_freq
    cos, sin = jnp.cos(angles), jnp.sin(angles)
    return jnp.concatenate([cos, cos], axis=-1), jnp.concatenate([-sin, sin], axis=-1)


def qkv_kernel(head_dim, rope_heads, a_ref, w_ref, cos_ref, sin_ref, o_ref):
    cols = w_ref.shape[1]
    step = 4 * head_dim
    cos, sin = cos_ref[...], sin_ref[...]
    for start in range(0, cols, step):
        proj = jnp.dot(a_ref[...], w_ref[:, start:start + step], preferred_element_type=F32)
        for k in range(step // head_dim):
            x = proj[:, k * head_dim:(k + 1) * head_dim]
            if start // head_dim + k < rope_heads:
                x = x * cos + pltpu.roll(x, head_dim // 2, 1) * sin
            o_ref[:, start + k * head_dim:start + (k + 1) * head_dim] = x.astype(BF16)


def project_qkv(a, w, cos, sin, rope_heads):
    tokens, d_model = a.shape
    cols, head_dim = w.shape[1], cos.shape[1]
    rows = min(256, tokens)
    return pl.pallas_call(
        functools.partial(qkv_kernel, head_dim, rope_heads),
        grid=(tokens // rows,),
        out_shape=jax.ShapeDtypeStruct((tokens, cols), BF16),
        in_specs=[
            pl.BlockSpec((rows, d_model), lambda i: (i, 0)),
            pl.BlockSpec((d_model, cols), lambda i: (0, 0), pipeline_mode=pl.Buffered(1)),
            pl.BlockSpec((rows, head_dim), lambda i: (i, 0)),
            pl.BlockSpec((rows, head_dim), lambda i: (i, 0)),
        ],
        out_specs=pl.BlockSpec((rows, cols), lambda i: (i, 0)),
        compiler_params=pltpu.CompilerParams(vmem_limit_bytes=VMEM_BIG),
        cost_estimate=pl.CostEstimate(flops=2 * tokens * d_model * cols, bytes_accessed=2 * (tokens * d_model + d_model * cols + tokens * cols), transcendentals=0),
        name="qkv",
    )(a, w, cos, sin)


def attn_kernel(group, head_dim, per_seg, table_ref, q_ref, k_ref, v_ref, o_ref, m_sc, l_sc, acc_sc):
    blk = q_ref.shape[0]
    seg_rows = per_seg * blk
    qi = pl.program_id(1)
    true_seg = table_ref[4 + qi // per_seg]
    n_full = true_seg * per_seg + lax.rem(qi, per_seg)
    scale = (head_dim ** -0.5) * 1.4426950408889634
    m_sc[...] = jnp.full(m_sc.shape, -1e30, F32)
    l_sc[...] = jnp.zeros(l_sc.shape, F32)
    acc_sc[...] = jnp.zeros(acc_sc.shape, F32)

    def step(j, masked):
        row = table_ref[j // per_seg] * seg_rows + lax.rem(j, per_seg) * blk
        rows = pl.ds(pl.multiple_of(row, blk), blk)
        k, v = k_ref[rows, :], v_ref[rows, :]
        for h in range(group):
            q = q_ref[:, h * head_dim:(h + 1) * head_dim]
            s = lax.dot_general(q, k, (((1,), (1,)), ((), ())), preferred_element_type=F32)
            if masked:
                keep = lax.broadcasted_iota(jnp.int32, s.shape, 0) >= lax.broadcasted_iota(jnp.int32, s.shape, 1)
                s = jnp.where(keep, s, -1e30)
            m_old = m_sc[h, :, 0:1]
            m_new = jnp.maximum(m_old, jnp.max(s, axis=1, keepdims=True))
            alpha = jnp.exp2((m_old - m_new) * scale)
            p = jnp.exp2((s - m_new) * scale)
            part = p[:, 0:128]
            for c in range(128, blk, 128):
                part = part + p[:, c:c + 128]
            l_sc[h] = l_sc[h] * alpha + part
            acc_sc[h] = acc_sc[h] * alpha + jnp.dot(p.astype(BF16), v, preferred_element_type=F32)
            m_sc[h] = jnp.broadcast_to(m_new, m_sc.shape[1:])

    def body(j, carry):
        step(j, False)
        return carry

    lax.fori_loop(0, n_full, body, 0)
    step(n_full, True)
    for h in range(group):
        total = jnp.sum(l_sc[h], axis=1, keepdims=True)
        o_ref[:, h * head_dim:(h + 1) * head_dim] = (acc_sc[h] / total).astype(BF16)


def attention(qkv, kv_all, table, heads, kv_heads, head_dim):
    tokens, keys = qkv.shape[0], kv_all.shape[0]
    seg_rows = tokens // 2
    blk = min(256, seg_rows)
    per_seg = seg_rows // blk
    group = heads // kv_heads
    return pl.pallas_call(
        functools.partial(attn_kernel, group, head_dim, per_seg),
        grid_spec=pltpu.PrefetchScalarGridSpec(
            num_scalar_prefetch=1,
            grid=(kv_heads, tokens // blk),
            in_specs=[
                pl.BlockSpec((blk, group * head_dim), lambda g, i, t: (i, g)),
                pl.BlockSpec((keys, head_dim), lambda g, i, t: (0, g)),
                pl.BlockSpec((keys, head_dim), lambda g, i, t: (0, kv_heads + g)),
            ],
            out_specs=pl.BlockSpec((blk, group * head_dim), lambda g, i, t: (i, g)),
            scratch_shapes=[pltpu.VMEM((group, blk, 128), F32), pltpu.VMEM((group, blk, 128), F32), pltpu.VMEM((group, blk, head_dim), F32)],
        ),
        out_shape=jax.ShapeDtypeStruct((tokens, heads * head_dim), BF16),
        compiler_params=pltpu.CompilerParams(vmem_limit_bytes=32 * 1024 * 1024),
        cost_estimate=pl.CostEstimate(flops=2 * tokens * keys * heads * head_dim * 2, bytes_accessed=2 * (2 * tokens * heads * head_dim + 4 * keys * head_dim), transcendentals=tokens * keys * heads),
        name="attn",
    )(table, qkv, kv_all, kv_all)


def sum_kernel(n_tp, col_off, with_norm, n_after, lhs_hbm, w_hbm, res_hbm, gain_ref, *refs):
    refs = refs[n_after:]
    if with_norm:
        own_hbm, out_hbm = refs[:2]
        refs = refs[2:]
    else:
        out_hbm = refs[0]
        refs = refs[1:]
    lhs, w, part, in1, in2, res, own, norm, w_sem, l_sem, r_sem, o_sem, s1, r1, s2, r2, s3, r3, s4, r4 = refs
    n_w, depth, n_cols = w.shape
    cols = n_w * n_cols
    half = cols // 2
    rows = part.shape[2]
    block = rows * N_SUB
    me = lax.axis_index("tp")
    right, left = lax.rem(me + 1, n_tp), lax.rem(me + n_tp - 1, n_tp)
    far = lax.rem(me + 2, n_tp)
    sides = (right, left)
    lo, hi = pl.ds(0, half), pl.ds(half, half)
    halves = (lo, hi)

    def w_copy(d):
        return pltpu.make_async_copy(w_hbm.at[d], w.at[d], w_sem.at[d])

    lhs_copies = [pltpu.make_async_copy(lhs_hbm.at[pl.ds(b * block, block), :], lhs.at[b], l_sem.at[b]) for b in range(n_tp)]
    for c in lhs_copies:
        c.start()
    for d in range(n_w):
        w_copy(d).start()
    my_rows = pl.ds(pl.multiple_of(me * block, block), block)
    if with_norm:
        res_copies = [pltpu.make_async_copy(res_hbm.at[my_rows, :], res, r_sem.at[0])]
    else:
        wide = res_hbm.shape[1] // n_w
        res_copies = [pltpu.make_async_copy(res_hbm.at[:, pl.ds(d * wide + col_off, n_cols)], res.at[:, pl.ds(d * n_cols, n_cols)], r_sem.at[d]) for d in range(n_w)]
    for c in res_copies:
        c.start()

    barrier = pltpu.get_barrier_semaphore()
    for dev in sides:
        pl.semaphore_signal(barrier, inc=1, device_id={"tp": dev}, device_id_type=MESH)
    pl.semaphore_wait(barrier, 2)

    def remote(src, dst, send, recv, dev):
        return pltpu.make_async_remote_copy(src_ref=src, dst_ref=dst, send_sem=send, recv_sem=recv, device_id={"tp": dev}, device_id_type=MESH)

    def rows_of(b, s):
        return pl.ds(pl.multiple_of(b * block + s * rows, rows), rows)

    def hop1(s, i):
        return remote(part.at[s, far, :, halves[i]], in1.at[s, i], s1.at[s, i], r1.at[s, i], sides[i])

    def hop2(s, i):
        return remote(part.at[s, sides[i]], in2.at[s, i], s2.at[s, i], r2.at[s, i], sides[i])

    def hop3(s, i):
        return remote(norm.at[s], out_hbm.at[rows_of(me, s), :], s3.at[s, i], r3.at[s, i], sides[i])

    def hop4(s, i):
        block_rows = rows_of(sides[1 - i], s)
        where = out_hbm.at[block_rows, halves[i]]
        return remote(where, where, s4.at[s, i], r4.at[s, i], sides[i])

    def stage_a(s):
        left_rows = lhs[:, s * rows:(s + 1) * rows, :].reshape(n_tp * rows, depth)

        def one(d, carry):
            if s == 0:
                w_copy(d).wait()
            prod = jnp.dot(left_rows, w[d], preferred_element_type=F32).astype(BF16)
            part[s, :, :, pl.ds(pl.multiple_of(d * n_cols, n_cols), n_cols)] = prod.reshape(n_tp, rows, n_cols)
            return carry

        lax.fori_loop(0, n_w, one, 0)
        for i in range(2):
            hop1(s, i).start()

    def stage_b(s):
        for i in range(2):
            hop1(s, i).wait_recv()
            dest = sides[i]
            mine = part[s, dest, :, halves[i]].astype(F32)
            part[s, dest, :, halves[i]] = (mine + in1[s, i].astype(F32)).astype(BF16)
            hop2(s, i).start()

    def stage_c(s):
        for i in range(2):
            hop2(s, i).wait_recv()
        step = 16

        def one(k, carry):
            at = pl.ds(pl.multiple_of(k * step, step), step)
            total = part[s, me, at, :].astype(F32) + in2[s, 0, at, :].astype(F32) + in2[s, 1, at, :].astype(F32)
            total = total.astype(BF16).astype(F32)
            res_at = pl.ds(pl.multiple_of(s * rows + k * step, step), step)
            mid = (res[res_at, :].astype(F32) + total).astype(BF16)
            if with_norm:
                own[s, at, :] = mid
                mid = mid.astype(F32)
                mean_sq = jnp.mean(mid * mid, axis=-1, keepdims=True)
                mid = (mid * lax.rsqrt(mean_sq + NORM_EPS) * gain_ref[...]).astype(BF16)
            norm[s, at, :] = mid
            return carry

        lax.fori_loop(0, rows // step, one, 0)
        for i in range(2):
            hop3(s, i).start()
        local(s).start()
        if with_norm:
            keep(s).start()

    def local(s):
        return pltpu.make_async_copy(norm.at[s], out_hbm.at[rows_of(me, s), :], o_sem.at[s, 0])

    def keep(s):
        return pltpu.make_async_copy(own.at[s], own_hbm.at[pl.ds(s * rows, rows), :], o_sem.at[s, 1])

    def arrive3(s, i):
        where = out_hbm.at[rows_of(sides[1 - i], s), :]
        return remote(norm.at[s], where, s3.at[s, i], r3.at[s, i], sides[i])

    def arrive4(s, i):
        where = out_hbm.at[rows_of(far, s), halves[i]]
        return remote(where, where, s4.at[s, i], r4.at[s, i], sides[i])

    def stage_d(s):
        for i in range(2):
            arrive3(s, i).wait_recv()
            hop4(s, i).start()

    for c in lhs_copies:
        c.wait()
    for t in range(N_SUB + 3):
        if t < N_SUB:
            stage_a(t)
        if 0 <= t - 1 < N_SUB:
            stage_b(t - 1)
        if t == 1:
            for c in res_copies:
                c.wait()
        if 0 <= t - 2 < N_SUB:
            stage_c(t - 2)
        if 0 <= t - 3 < N_SUB:
            stage_d(t - 3)
    for s in range(N_SUB):
        local(s).wait()
        if with_norm:
            keep(s).wait()
        for i in range(2):
            hop1(s, i).wait_send()
            hop2(s, i).wait_send()
            hop3(s, i).wait_send()
            hop4(s, i).wait_send()
            arrive4(s, i).wait_recv()


def sum_over_tp(n_tp, lhs, w, res, gain, col_off, with_norm, collective_id, after=()):
    tokens, depth = lhs.shape
    n_w, _, n_cols = w.shape
    cols = n_w * n_cols
    block = tokens // n_tp
    rows = block // N_SUB
    out_shape = [jax.ShapeDtypeStruct((tokens, cols), BF16)]
    if with_norm:
        out_shape = [jax.ShapeDtypeStruct((block, cols), BF16)] + out_shape
    dma = pltpu.SemaphoreType.DMA
    small = (N_SUB, rows, cols) if with_norm else (1, 16, 128)
    scratch = [
        pltpu.VMEM((n_tp, block, depth), BF16),
        pltpu.VMEM((n_w, depth, n_cols), BF16),
        pltpu.VMEM((N_SUB, n_tp, rows, cols), BF16),
        pltpu.VMEM((N_SUB, 2, rows, cols // 2), BF16),
        pltpu.VMEM((N_SUB, 2, rows, cols), BF16),
        pltpu.VMEM((block, cols), BF16),
        pltpu.VMEM(small, BF16),
        pltpu.VMEM((N_SUB, rows, cols), BF16),
        dma((n_w,)), dma((n_tp,)), dma((n_w,)), dma((N_SUB, 2)),
    ] + [dma((N_SUB, 2))] * 8
    return pl.pallas_call(
        functools.partial(sum_kernel, n_tp, col_off, with_norm, len(after)),
        out_shape=out_shape,
        in_specs=[ANY, ANY, ANY, pl.BlockSpec(memory_space=pltpu.VMEM)] + [ANY] * len(after),
        out_specs=[ANY] * len(out_shape),
        scratch_shapes=scratch,
        compiler_params=pltpu.CompilerParams(collective_id=collective_id, has_side_effects=True, vmem_limit_bytes=VMEM_BIG),
        cost_estimate=pl.CostEstimate(flops=2 * tokens * cols * 30000, bytes_accessed=2 * (tokens * depth + depth * cols + 2 * tokens * cols), transcendentals=0),
        name="sum_tp_%d" % collective_id,
    )(lhs, w, res, gain, *after)


def join_kernel(n_w, a_ref, b_ref, o_ref):
    wa, wb = a_ref.shape[1] // n_w, b_ref.shape[1] // n_w
    for d in range(n_w):
        base = d * (wa + wb)
        o_ref[:, base:base + wa] = a_ref[:, d * wa:(d + 1) * wa]
        o_ref[:, base + wa:base + wa + wb] = b_ref[:, d * wb:(d + 1) * wb]


def join_columns(a, b, n_w):
    tokens = a.shape[0]
    rows = min(256, tokens)
    cols = a.shape[1] + b.shape[1]
    return pl.pallas_call(
        functools.partial(join_kernel, n_w),
        grid=(tokens // rows,),
        out_shape=jax.ShapeDtypeStruct((tokens, cols), BF16),
        in_specs=[pl.BlockSpec((rows, a.shape[1]), lambda i: (i, 0)), pl.BlockSpec((rows, b.shape[1]), lambda i: (i, 0))],
        out_specs=pl.BlockSpec((rows, cols), lambda i: (i, 0)),
        cost_estimate=pl.CostEstimate(flops=tokens * cols, bytes_accessed=4 * tokens * cols, transcendentals=0),
        name="join",
    )(a, b)


def solution(mesh):
    seq_spec = P(('dp', 'fsdp'), 'cp', None)
    pos_spec = P(('dp', 'fsdp'), 'cp')
    in_spec = P(GROUP_AXES, 'tp', None)
    out_spec = P('tp', None, GROUP_AXES)
    col_spec = P(GROUP_AXES, 'tp')
    row_spec = P('tp', GROUP_AXES)
    rep_spec = P(None)
    n_tp = mesh.shape['tp']
    n_w = mesh.shape['fsdp'] * mesh.shape['cp']

    def layer_local(hidden, positions, attn_gain, w_query, w_key, w_value, w_out, mlp_gain, w_gate, w_up, w_down):
        tokens, d_model = hidden.shape[1:]
        share, heads, head_dim = w_query.shape
        kv_heads = w_key.shape[1]
        w_qkv = jnp.concatenate([w.reshape(share, -1) for w in (w_query, w_key, w_value)], axis=1)
        full_qkv = lax.all_gather(w_qkv, GROUP_AXES, axis=0, tiled=True)
        full_out = lax.all_gather(w_out.reshape(heads * head_dim, share), GROUP_AXES, axis=0, tiled=False)
        full_gate = lax.all_gather(w_gate, GROUP_AXES, axis=0, tiled=True)
        full_up = lax.all_gather(w_up, GROUP_AXES, axis=0, tiled=True)
        cut = (share * 2 // 5) // 128 * 128
        full_down0 = lax.all_gather(w_down[:, :cut], GROUP_AXES, axis=0, tiled=False)
        full_down1 = lax.all_gather(w_down[:, cut:], GROUP_AXES, axis=0, tiled=False)

        x = hidden[0]
        normed = rms_norm(x.astype(F32), attn_gain)
        cos, sin = rope_tables(positions[0], head_dim)
        qkv = project_qkv(normed, full_qkv, cos, sin, heads + kv_heads)
        kv = qkv[:, heads * head_dim:]
        kv_peer = lax.ppermute(kv, 'cp', [(0, 1), (1, 0)])
        c = lax.axis_index('cp')
        table = jnp.where(c == 0, jnp.array([0, 2, 3, 1, 0, 3], jnp.int32), jnp.array([2, 0, 1, 3, 1, 2], jnp.int32))
        kv_all = jnp.concatenate([kv, kv_peer], axis=0)
        mixed = attention(qkv, kv_all, table, heads, kv_heads, head_dim)
        mid_own, normed_mlp = sum_over_tp(n_tp, mixed, full_out, x, attn_gain_row(mlp_gain), 0, True, 0)
        gate_proj = jnp.dot(normed_mlp, full_gate, preferred_element_type=F32)
        up_proj = jnp.dot(normed_mlp, full_up, preferred_element_type=F32)
        act = (jax.nn.silu(gate_proj) * up_proj).astype(BF16)
        piece0, = sum_over_tp(n_tp, act, full_down0, mid_own, attn_gain_row(mlp_gain), 0, False, 1)
        piece1, = sum_over_tp(n_tp, act, full_down1, mid_own, attn_gain_row(mlp_gain), cut, False, 2, after=(piece0,))
        return join_columns(piece0, piece1, n_w)[None]

    return jax.shard_map(layer_local, mesh=mesh, in_specs=(seq_spec, pos_spec, rep_spec, in_spec, in_spec, in_spec, out_spec, rep_spec, col_spec, col_spec, row_spec), out_specs=seq_spec, check_vma=False)


def attn_gain_row(gain):
    return gain[None, :]
```

```python
import functools

import jax
import jax.numpy as jnp
from jax import lax
from jax.experimental import pallas as pl
from jax.experimental.pallas import tpu as pltpu
from jax.sharding import PartitionSpec as P

ROPE_THETA = 500000.0
NORM_EPS = 1e-5
GROUP_AXES = ('fsdp', 'cp')
N_SUB = 4
F32 = jnp.float32
BF16 = jnp.bfloat16
MESH = pl.DeviceIdType.MESH
VMEM_BIG = 58 * 1024 * 1024
ANY = pl.BlockSpec(memory_space=pl.ANY)


def rms_norm(hidden_f32, gain):
    mean_sq = jnp.mean(hidden_f32 * hidden_f32, axis=-1, keepdims=True)
    return (hidden_f32 * lax.rsqrt(mean_sq + NORM_EPS) * gain).astype(BF16)


def rope_tables(positions, head_dim):
    inv_freq = ROPE_THETA ** (-jnp.arange(0, head_dim, 2, dtype=F32) / head_dim)
    angles = positions.astype(F32)[..., None] * inv_freq
    cos, sin = jnp.cos(angles), jnp.sin(angles)
    return jnp.concatenate([cos, cos], axis=-1), jnp.concatenate([-sin, sin], axis=-1)


def qkv_kernel(head_dim, rope_heads, a_ref, w_ref, cos_ref, sin_ref, o_ref):
    cols = w_ref.shape[1]
    step = 4 * head_dim
    cos, sin = cos_ref[...], sin_ref[...]
    for start in range(0, cols, step):
        proj = jnp.dot(a_ref[...], w_ref[:, start:start + step], preferred_element_type=F32)
        for k in range(step // head_dim):
            x = proj[:, k * head_dim:(k + 1) * head_dim]
            if start // head_dim + k < rope_heads:
                x = x * cos + pltpu.roll(x, head_dim // 2, 1) * sin
            o_ref[:, start + k * head_dim:start + (k + 1) * head_dim] = x.astype(BF16)


def project_qkv(a, w, cos, sin, rope_heads):
    tokens, d_model = a.shape
    cols, head_dim = w.shape[1], cos.shape[1]
    rows = min(256, tokens)
    return pl.pallas_call(
        functools.partial(qkv_kernel, head_dim, rope_heads),
        grid=(tokens // rows,),
        out_shape=jax.ShapeDtypeStruct((tokens, cols), BF16),
        in_specs=[
            pl.BlockSpec((rows, d_model), lambda i: (i, 0)),
            pl.BlockSpec((d_model, cols), lambda i: (0, 0), pipeline_mode=pl.Buffered(1)),
            pl.BlockSpec((rows, head_dim), lambda i: (i, 0)),
            pl.BlockSpec((rows, head_dim), lambda i: (i, 0)),
        ],
        out_specs=pl.BlockSpec((rows, cols), lambda i: (i, 0)),
        compiler_params=pltpu.CompilerParams(vmem_limit_bytes=VMEM_BIG),
        cost_estimate=pl.CostEstimate(flops=2 * tokens * d_model * cols, bytes_accessed=2 * (tokens * d_model + d_model * cols + tokens * cols), transcendentals=0),
        name="qkv",
    )(a, w, cos, sin)


def attn_kernel(group, head_dim, per_seg, table_ref, q_ref, k_ref, vt_ref, o_ref, m_sc, l_sc, acc_sc):
    blk = q_ref.shape[0]
    seg_rows = per_seg * blk
    qi = pl.program_id(1)
    true_seg = table_ref[4 + qi // per_seg]
    n_full = true_seg * per_seg + lax.rem(qi, per_seg)
    scale = (head_dim ** -0.5) * 1.4426950408889634
    m_sc[...] = jnp.full(m_sc.shape, -1e30, F32)
    l_sc[...] = jnp.zeros(l_sc.shape, F32)
    acc_sc[...] = jnp.zeros(acc_sc.shape, F32)

    def step(j, masked):
        row = table_ref[j // per_seg] * seg_rows + lax.rem(j, per_seg) * blk
        rows = pl.ds(pl.multiple_of(row, blk), blk)
        k, vt = k_ref[rows, :], vt_ref[:, rows]
        for h in range(group):
            q = q_ref[:, h * head_dim:(h + 1) * head_dim]
            s = lax.dot_general(k, q, (((1,), (1,)), ((), ())), preferred_element_type=F32) * scale
            if masked:
                keep = lax.broadcasted_iota(jnp.int32, s.shape, 0) <= lax.broadcasted_iota(jnp.int32, s.shape, 1)
                s = jnp.where(keep, s, -1e30)
            m_old = m_sc[h]
            m_new = jnp.maximum(m_old, jnp.max(s, axis=0, keepdims=True))
            alpha = jnp.exp2(m_old - m_new)
            p = jnp.exp2(s - m_new)
            l_sc[h] = l_sc[h] * alpha + jnp.sum(p, axis=0, keepdims=True)
            acc_sc[h] = acc_sc[h] * alpha + jnp.dot(vt, p.astype(BF16), preferred_element_type=F32)
            m_sc[h] = m_new

    def body(j, carry):
        step(j, False)
        return carry

    lax.fori_loop(0, n_full, body, 0)
    step(n_full, True)
    for h in range(group):
        o_ref[:, h * head_dim:(h + 1) * head_dim] = (acc_sc[h] / l_sc[h]).T.astype(BF16)


def attention(qkv, k_all, vt_all, table, heads, kv_heads, head_dim):
    tokens, keys = qkv.shape[0], k_all.shape[0]
    seg_rows = tokens // 2
    blk = min(256, seg_rows)
    per_seg = seg_rows // blk
    group = heads // kv_heads
    return pl.pallas_call(
        functools.partial(attn_kernel, group, head_dim, per_seg),
        grid_spec=pltpu.PrefetchScalarGridSpec(
            num_scalar_prefetch=1,
            grid=(kv_heads, tokens // blk),
            in_specs=[
                pl.BlockSpec((blk, group * head_dim), lambda g, i, t: (i, g)),
                pl.BlockSpec((keys, head_dim), lambda g, i, t: (0, g)),
                pl.BlockSpec((head_dim, keys), lambda g, i, t: (g, 0)),
            ],
            out_specs=pl.BlockSpec((blk, group * head_dim), lambda g, i, t: (i, g)),
            scratch_shapes=[pltpu.VMEM((group, 1, blk), F32), pltpu.VMEM((group, 1, blk), F32), pltpu.VMEM((group, head_dim, blk), F32)],
        ),
        out_shape=jax.ShapeDtypeStruct((tokens, heads * head_dim), BF16),
        compiler_params=pltpu.CompilerParams(vmem_limit_bytes=32 * 1024 * 1024),
        cost_estimate=pl.CostEstimate(flops=2 * tokens * keys * heads * head_dim * 2, bytes_accessed=2 * (2 * tokens * heads * head_dim + 4 * keys * head_dim), transcendentals=tokens * keys * heads),
        name="attn",
    )(table, qkv, k_all, vt_all)


def sum_kernel(n_tp, col_off, with_norm, n_after, lhs_hbm, w_hbm, res_hbm, gain_ref, *refs):
    refs = refs[n_after:]
    if with_norm:
        own_hbm, out_hbm = refs[:2]
        refs = refs[2:]
    else:
        out_hbm = refs[0]
        refs = refs[1:]
    lhs, w, part, in1, in2, res, own, norm, w_sem, l_sem, r_sem, o_sem, s1, r1, s2, r2, s3, r3, s4, r4 = refs
    n_w, depth, n_cols = w.shape
    cols = n_w * n_cols
    half = cols // 2
    rows = part.shape[2]
    block = rows * N_SUB
    me = lax.axis_index("tp")
    right, left = lax.rem(me + 1, n_tp), lax.rem(me + n_tp - 1, n_tp)
    far = lax.rem(me + 2, n_tp)
    sides = (right, left)
    lo, hi = pl.ds(0, half), pl.ds(half, half)
    halves = (lo, hi)

    def w_copy(d):
        return pltpu.make_async_copy(w_hbm.at[d], w.at[d], w_sem.at[d])

    lhs_copies = [pltpu.make_async_copy(lhs_hbm.at[pl.ds(b * block, block), :], lhs.at[b], l_sem.at[b]) for b in range(n_tp)]
    for c in lhs_copies:
        c.start()
    for d in range(n_w):
        w_copy(d).start()
    my_rows = pl.ds(pl.multiple_of(me * block, block), block)
    if with_norm:
        res_copies = [pltpu.make_async_copy(res_hbm.at[my_rows, :], res, r_sem.at[0])]
    else:
        wide = res_hbm.shape[1] // n_w
        res_copies = [pltpu.make_async_copy(res_hbm.at[:, pl.ds(d * wide + col_off, n_cols)], res.at[:, pl.ds(d * n_cols, n_cols)], r_sem.at[d]) for d in range(n_w)]
    for c in res_copies:
        c.start()

    barrier = pltpu.get_barrier_semaphore()
    for dev in sides:
        pl.semaphore_signal(barrier, inc=1, device_id={"tp": dev}, device_id_type=MESH)
    pl.semaphore_wait(barrier, 2)

    def remote(src, dst, send, recv, dev):
        return pltpu.make_async_remote_copy(src_ref=src, dst_ref=dst, send_sem=send, recv_sem=recv, device_id={"tp": dev}, device_id_type=MESH)

    def rows_of(b, s):
        return pl.ds(pl.multiple_of(b * block + s * rows, rows), rows)

    def hop1(s, i):
        return remote(part.at[s, far, :, halves[i]], in1.at[s, i], s1.at[s, i], r1.at[s, i], sides[i])

    def hop2(s, i):
        return remote(part.at[s, sides[i]], in2.at[s, i], s2.at[s, i], r2.at[s, i], sides[i])

    def hop3(s, i):
        return remote(norm.at[s], out_hbm.at[rows_of(me, s), :], s3.at[s, i], r3.at[s, i], sides[i])

    def hop4(s, i):
        block_rows = rows_of(sides[1 - i], s)
        where = out_hbm.at[block_rows, halves[i]]
        return remote(where, where, s4.at[s, i], r4.at[s, i], sides[i])

    def stage_a(s):
        left_rows = lhs[:, s * rows:(s + 1) * rows, :].reshape(n_tp * rows, depth)

        def one(d, carry):
            if s == 0:
                w_copy(d).wait()
            prod = jnp.dot(left_rows, w[d], preferred_element_type=F32).astype(BF16)
            part[s, :, :, pl.ds(pl.multiple_of(d * n_cols, n_cols), n_cols)] = prod.reshape(n_tp, rows, n_cols)
            return carry

        lax.fori_loop(0, n_w, one, 0)
        for i in range(2):
            hop1(s, i).start()

    def stage_b(s):
        for i in range(2):
            hop1(s, i).wait_recv()
            dest = sides[i]
            mine = part[s, dest, :, halves[i]].astype(F32)
            part[s, dest, :, halves[i]] = (mine + in1[s, i].astype(F32)).astype(BF16)
            hop2(s, i).start()

    def stage_c(s):
        for i in range(2):
            hop2(s, i).wait_recv()
        step = 16

        def one(k, carry):
            at = pl.ds(pl.multiple_of(k * step, step), step)
            total = part[s, me, at, :].astype(F32) + in2[s, 0, at, :].astype(F32) + in2[s, 1, at, :].astype(F32)
            total = total.astype(BF16).astype(F32)
            res_at = pl.ds(pl.multiple_of(s * rows + k * step, step), step)
            mid = (res[res_at, :].astype(F32) + total).astype(BF16)
            if with_norm:
                own[s, at, :] = mid
                mid = mid.astype(F32)
                mean_sq = jnp.mean(mid * mid, axis=-1, keepdims=True)
                mid = (mid * lax.rsqrt(mean_sq + NORM_EPS) * gain_ref[...]).astype(BF16)
            norm[s, at, :] = mid
            return carry

        lax.fori_loop(0, rows // step, one, 0)
        for i in range(2):
            hop3(s, i).start()
        local(s).start()
        if with_norm:
            keep(s).start()

    def local(s):
        return pltpu.make_async_copy(norm.at[s], out_hbm.at[rows_of(me, s), :], o_sem.at[s, 0])

    def keep(s):
        return pltpu.make_async_copy(own.at[s], own_hbm.at[pl.ds(s * rows, rows), :], o_sem.at[s, 1])

    def arrive3(s, i):
        where = out_hbm.at[rows_of(sides[1 - i], s), :]
        return remote(norm.at[s], where, s3.at[s, i], r3.at[s, i], sides[i])

    def arrive4(s, i):
        where = out_hbm.at[rows_of(far, s), halves[i]]
        return remote(where, where, s4.at[s, i], r4.at[s, i], sides[i])

    def stage_d(s):
        for i in range(2):
            arrive3(s, i).wait_recv()
            hop4(s, i).start()

    for c in lhs_copies:
        c.wait()
    for t in range(N_SUB + 3):
        if t < N_SUB:
            stage_a(t)
        if 0 <= t - 1 < N_SUB:
            stage_b(t - 1)
        if t == 1:
            for c in res_copies:
                c.wait()
        if 0 <= t - 2 < N_SUB:
            stage_c(t - 2)
        if 0 <= t - 3 < N_SUB:
            stage_d(t - 3)
    for s in range(N_SUB):
        local(s).wait()
        if with_norm:
            keep(s).wait()
        for i in range(2):
            hop1(s, i).wait_send()
            hop2(s, i).wait_send()
            hop3(s, i).wait_send()
            hop4(s, i).wait_send()
            arrive4(s, i).wait_recv()


def sum_over_tp(n_tp, lhs, w, res, gain, col_off, with_norm, collective_id, after=()):
    tokens, depth = lhs.shape
    n_w, _, n_cols = w.shape
    cols = n_w * n_cols
    block = tokens // n_tp
    rows = block // N_SUB
    out_shape = [jax.ShapeDtypeStruct((tokens, cols), BF16)]
    if with_norm:
        out_shape = [jax.ShapeDtypeStruct((block, cols), BF16)] + out_shape
    dma = pltpu.SemaphoreType.DMA
    small = (N_SUB, rows, cols) if with_norm else (1, 16, 128)
    scratch = [
        pltpu.VMEM((n_tp, block, depth), BF16),
        pltpu.VMEM((n_w, depth, n_cols), BF16),
        pltpu.VMEM((N_SUB, n_tp, rows, cols), BF16),
        pltpu.VMEM((N_SUB, 2, rows, cols // 2), BF16),
        pltpu.VMEM((N_SUB, 2, rows, cols), BF16),
        pltpu.VMEM((block, cols), BF16),
        pltpu.VMEM(small, BF16),
        pltpu.VMEM((N_SUB, rows, cols), BF16),
        dma((n_w,)), dma((n_tp,)), dma((n_w,)), dma((N_SUB, 2)),
    ] + [dma((N_SUB, 2))] * 8
    return pl.pallas_call(
        functools.partial(sum_kernel, n_tp, col_off, with_norm, len(after)),
        out_shape=out_shape,
        in_specs=[ANY, ANY, ANY, pl.BlockSpec(memory_space=pltpu.VMEM)] + [ANY] * len(after),
        out_specs=[ANY] * len(out_shape),
        scratch_shapes=scratch,
        compiler_params=pltpu.CompilerParams(collective_id=collective_id, has_side_effects=True, vmem_limit_bytes=VMEM_BIG),
        cost_estimate=pl.CostEstimate(flops=2 * tokens * cols * 30000, bytes_accessed=2 * (tokens * depth + depth * cols + 2 * tokens * cols), transcendentals=0),
        name="sum_tp_%d" % collective_id,
    )(lhs, w, res, gain, *after)


def join_kernel(n_w, a_ref, b_ref, o_ref):
    wa, wb = a_ref.shape[1] // n_w, b_ref.shape[1] // n_w
    for d in range(n_w):
        base = d * (wa + wb)
        o_ref[:, base:base + wa] = a_ref[:, d * wa:(d + 1) * wa]
        o_ref[:, base + wa:base + wa + wb] = b_ref[:, d * wb:(d + 1) * wb]


def join_columns(a, b, n_w):
    tokens = a.shape[0]
    rows = min(256, tokens)
    cols = a.shape[1] + b.shape[1]
    return pl.pallas_call(
        functools.partial(join_kernel, n_w),
        grid=(tokens // rows,),
        out_shape=jax.ShapeDtypeStruct((tokens, cols), BF16),
        in_specs=[pl.BlockSpec((rows, a.shape[1]), lambda i: (i, 0)), pl.BlockSpec((rows, b.shape[1]), lambda i: (i, 0))],
        out_specs=pl.BlockSpec((rows, cols), lambda i: (i, 0)),
        cost_estimate=pl.CostEstimate(flops=tokens * cols, bytes_accessed=4 * tokens * cols, transcendentals=0),
        name="join",
    )(a, b)


def solution(mesh):
    seq_spec = P(('dp', 'fsdp'), 'cp', None)
    pos_spec = P(('dp', 'fsdp'), 'cp')
    in_spec = P(GROUP_AXES, 'tp', None)
    out_spec = P('tp', None, GROUP_AXES)
    col_spec = P(GROUP_AXES, 'tp')
    row_spec = P('tp', GROUP_AXES)
    rep_spec = P(None)
    n_tp = mesh.shape['tp']
    n_w = mesh.shape['fsdp'] * mesh.shape['cp']

    def layer_local(hidden, positions, attn_gain, w_query, w_key, w_value, w_out, mlp_gain, w_gate, w_up, w_down):
        tokens, d_model = hidden.shape[1:]
        share, heads, head_dim = w_query.shape
        kv_heads = w_key.shape[1]
        w_qkv = jnp.concatenate([w.reshape(share, -1) for w in (w_query, w_key, w_value)], axis=1)
        full_qkv = lax.all_gather(w_qkv, GROUP_AXES, axis=0, tiled=True)
        full_out = lax.all_gather(w_out.reshape(heads * head_dim, share), GROUP_AXES, axis=0, tiled=False)
        full_gate = lax.all_gather(w_gate, GROUP_AXES, axis=0, tiled=True)
        full_up = lax.all_gather(w_up, GROUP_AXES, axis=0, tiled=True)
        cut = (share * 2 // 5) // 128 * 128
        full_down0 = lax.all_gather(w_down[:, :cut], GROUP_AXES, axis=0, tiled=False)
        full_down1 = lax.all_gather(w_down[:, cut:], GROUP_AXES, axis=0, tiled=False)

        x = hidden[0]
        normed = rms_norm(x.astype(F32), attn_gain)
        cos, sin = rope_tables(positions[0], head_dim)
        qkv = project_qkv(normed, full_qkv, cos, sin, heads + kv_heads)
        kv = qkv[:, heads * head_dim:]
        kv_peer = lax.ppermute(kv, 'cp', [(0, 1), (1, 0)])
        c = lax.axis_index('cp')
        table = jnp.where(c == 0, jnp.array([0, 2, 3, 1, 0, 3], jnp.int32), jnp.array([2, 0, 1, 3, 1, 2], jnp.int32))
        kv_all = jnp.concatenate([kv, kv_peer], axis=0)
        k_all, vt_all = kv_all[:, :kv_heads * head_dim], kv_all[:, kv_heads * head_dim:].T
        mixed = attention(qkv, k_all, vt_all, table, heads, kv_heads, head_dim)
        mid_own, normed_mlp = sum_over_tp(n_tp, mixed, full_out, x, attn_gain_row(mlp_gain), 0, True, 0)
        gate_proj = jnp.dot(normed_mlp, full_gate, preferred_element_type=F32)
        up_proj = jnp.dot(normed_mlp, full_up, preferred_element_type=F32)
        act = (jax.nn.silu(gate_proj) * up_proj).astype(BF16)
        piece0, = sum_over_tp(n_tp, act, full_down0, mid_own, attn_gain_row(mlp_gain), 0, False, 1)
        piece1, = sum_over_tp(n_tp, act, full_down1, mid_own, attn_gain_row(mlp_gain), cut, False, 2, after=(piece0,))
        return join_columns(piece0, piece1, n_w)[None]

    return jax.shard_map(layer_local, mesh=mesh, in_specs=(seq_spec, pos_spec, rep_spec, in_spec, in_spec, in_spec, out_spec, rep_spec, col_spec, col_spec, row_spec), out_specs=seq_spec, check_vma=False)


def attn_gain_row(gain):
    return gain[None, :]
```

```python
import functools

import jax
import jax.numpy as jnp
from jax import lax
from jax.experimental import pallas as pl
from jax.experimental.pallas import tpu as pltpu
from jax.sharding import PartitionSpec as P

ROPE_THETA = 500000.0
NORM_EPS = 1e-5
GROUP_AXES = ('fsdp', 'cp')
N_SUB = 6
F32 = jnp.float32
BF16 = jnp.bfloat16
MESH = pl.DeviceIdType.MESH
VMEM_BIG = 58 * 1024 * 1024
ANY = pl.BlockSpec(memory_space=pl.ANY)


def rms_norm(hidden_f32, gain):
    mean_sq = jnp.mean(hidden_f32 * hidden_f32, axis=-1, keepdims=True)
    return (hidden_f32 * lax.rsqrt(mean_sq + NORM_EPS) * gain).astype(BF16)


def rope_tables(positions, head_dim):
    inv_freq = ROPE_THETA ** (-jnp.arange(0, head_dim, 2, dtype=F32) / head_dim)
    angles = positions.astype(F32)[..., None] * inv_freq
    cos, sin = jnp.cos(angles), jnp.sin(angles)
    return jnp.concatenate([cos, cos], axis=-1), jnp.concatenate([-sin, sin], axis=-1)


def qkv_kernel(head_dim, rope_heads, a_ref, w_ref, cos_ref, sin_ref, o_ref):
    cols = w_ref.shape[1]
    step = 4 * head_dim
    cos, sin = cos_ref[...], sin_ref[...]
    for start in range(0, cols, step):
        proj = jnp.dot(a_ref[...], w_ref[:, start:start + step], preferred_element_type=F32)
        for k in range(step // head_dim):
            x = proj[:, k * head_dim:(k + 1) * head_dim]
            if start // head_dim + k < rope_heads:
                x = x * cos + pltpu.roll(x, head_dim // 2, 1) * sin
            o_ref[:, start + k * head_dim:start + (k + 1) * head_dim] = x.astype(BF16)


def project_qkv(a, w, cos, sin, rope_heads):
    tokens, d_model = a.shape
    cols, head_dim = w.shape[1], cos.shape[1]
    rows = min(256, tokens)
    return pl.pallas_call(
        functools.partial(qkv_kernel, head_dim, rope_heads),
        grid=(tokens // rows,),
        out_shape=jax.ShapeDtypeStruct((tokens, cols), BF16),
        in_specs=[
            pl.BlockSpec((rows, d_model), lambda i: (i, 0)),
            pl.BlockSpec((d_model, cols), lambda i: (0, 0), pipeline_mode=pl.Buffered(1)),
            pl.BlockSpec((rows, head_dim), lambda i: (i, 0)),
            pl.BlockSpec((rows, head_dim), lambda i: (i, 0)),
        ],
        out_specs=pl.BlockSpec((rows, cols), lambda i: (i, 0)),
        compiler_params=pltpu.CompilerParams(vmem_limit_bytes=VMEM_BIG),
        cost_estimate=pl.CostEstimate(flops=2 * tokens * d_model * cols, bytes_accessed=2 * (tokens * d_model + d_model * cols + tokens * cols), transcendentals=0),
        name="qkv",
    )(a, w, cos, sin)


def attn_kernel(group, head_dim, per_seg, table_ref, q_ref, k_ref, vt_ref, o_ref, m_sc, l_sc, acc_sc):
    blk = q_ref.shape[0]
    seg_rows = per_seg * blk
    qi = pl.program_id(1)
    true_seg = table_ref[4 + qi // per_seg]
    within = lax.rem(qi, per_seg) * blk
    scale = (head_dim ** -0.5) * 1.4426950408889634
    m_sc[...] = jnp.full(m_sc.shape, -1e30, F32)
    l_sc[...] = jnp.zeros(l_sc.shape, F32)
    acc_sc[...] = jnp.zeros(acc_sc.shape, F32)

    def step(j, masked):
        rows = pl.ds(pl.multiple_of(table_ref[j] * seg_rows, seg_rows), seg_rows)
        k, vt = k_ref[rows, :], vt_ref[:, rows]
        for h in range(group):
            q = q_ref[:, h * head_dim:(h + 1) * head_dim]
            s = lax.dot_general(k, q, (((1,), (1,)), ((), ())), preferred_element_type=F32) * scale
            if masked:
                keep = lax.broadcasted_iota(jnp.int32, s.shape, 0) <= lax.broadcasted_iota(jnp.int32, s.shape, 1) + within
                s = jnp.where(keep, s, -1e30)
            m_old = m_sc[h]
            m_new = jnp.maximum(m_old, jnp.max(s, axis=0, keepdims=True))
            alpha = jnp.exp2(m_old - m_new)
            p = jnp.exp2(s - m_new)
            l_sc[h] = l_sc[h] * alpha + jnp.sum(p, axis=0, keepdims=True)
            acc_sc[h] = acc_sc[h] * alpha + jnp.dot(vt, p.astype(BF16), preferred_element_type=F32)
            m_sc[h] = m_new

    def body(j, carry):
        step(j, False)
        return carry

    lax.fori_loop(0, true_seg, body, 0)
    step(true_seg, True)
    for h in range(group):
        o_ref[:, h * head_dim:(h + 1) * head_dim] = (acc_sc[h] / l_sc[h]).T.astype(BF16)


def attention(qkv, k_all, vt_all, table, heads, kv_heads, head_dim):
    tokens, keys = qkv.shape[0], k_all.shape[0]
    seg_rows = tokens // 2
    blk = min(256, seg_rows)
    per_seg = seg_rows // blk
    group = heads // kv_heads
    return pl.pallas_call(
        functools.partial(attn_kernel, group, head_dim, per_seg),
        grid_spec=pltpu.PrefetchScalarGridSpec(
            num_scalar_prefetch=1,
            grid=(kv_heads, tokens // blk),
            in_specs=[
                pl.BlockSpec((blk, group * head_dim), lambda g, i, t: (i, g)),
                pl.BlockSpec((keys, head_dim), lambda g, i, t: (0, g)),
                pl.BlockSpec((head_dim, keys), lambda g, i, t: (g, 0)),
            ],
            out_specs=pl.BlockSpec((blk, group * head_dim), lambda g, i, t: (i, g)),
            scratch_shapes=[pltpu.VMEM((group, 1, blk), F32), pltpu.VMEM((group, 1, blk), F32), pltpu.VMEM((group, head_dim, blk), F32)],
        ),
        out_shape=jax.ShapeDtypeStruct((tokens, heads * head_dim), BF16),
        compiler_params=pltpu.CompilerParams(vmem_limit_bytes=32 * 1024 * 1024),
        cost_estimate=pl.CostEstimate(flops=2 * tokens * keys * heads * head_dim * 2, bytes_accessed=2 * (2 * tokens * heads * head_dim + 4 * keys * head_dim), transcendentals=tokens * keys * heads),
        name="attn",
    )(table, qkv, k_all, vt_all)


def sum_kernel(n_tp, col_off, with_norm, n_after, lhs_hbm, w_hbm, res_hbm, gain_ref, *refs):
    refs = refs[n_after:]
    if with_norm:
        own_hbm, out_hbm = refs[:2]
        refs = refs[2:]
    else:
        out_hbm = refs[0]
        refs = refs[1:]
    lhs, w, part, in1, in2, res, own, norm, w_sem, l_sem, r_sem, o_sem, s1, r1, s2, r2, s3, r3, s4, r4 = refs
    n_w, depth, n_cols = w.shape
    cols = n_w * n_cols
    half = cols // 2
    rows = part.shape[2]
    block = rows * N_SUB
    me = lax.axis_index("tp")
    right, left = lax.rem(me + 1, n_tp), lax.rem(me + n_tp - 1, n_tp)
    far = lax.rem(me + 2, n_tp)
    sides = (right, left)
    lo, hi = pl.ds(0, half), pl.ds(half, half)
    halves = (lo, hi)

    def w_copy(d):
        return pltpu.make_async_copy(w_hbm.at[d], w.at[d], w_sem.at[d])

    lhs_copies = [pltpu.make_async_copy(lhs_hbm.at[pl.ds(b * block, block), :], lhs.at[b], l_sem.at[b]) for b in range(n_tp)]
    for c in lhs_copies:
        c.start()
    for d in range(n_w):
        w_copy(d).start()
    my_rows = pl.ds(pl.multiple_of(me * block, block), block)
    if with_norm:
        res_copies = [pltpu.make_async_copy(res_hbm.at[my_rows, :], res, r_sem.at[0])]
    else:
        wide = res_hbm.shape[1] // n_w
        res_copies = [pltpu.make_async_copy(res_hbm.at[:, pl.ds(d * wide + col_off, n_cols)], res.at[:, pl.ds(d * n_cols, n_cols)], r_sem.at[d]) for d in range(n_w)]
    for c in res_copies:
        c.start()

    barrier = pltpu.get_barrier_semaphore()
    for dev in sides:
        pl.semaphore_signal(barrier, inc=1, device_id={"tp": dev}, device_id_type=MESH)
    pl.semaphore_wait(barrier, 2)

    def remote(src, dst, send, recv, dev):
        return pltpu.make_async_remote_copy(src_ref=src, dst_ref=dst, send_sem=send, recv_sem=recv, device_id={"tp": dev}, device_id_type=MESH)

    def rows_of(b, s):
        return pl.ds(pl.multiple_of(b * block + s * rows, rows), rows)

    def hop1(s, i):
        return remote(part.at[s, far, :, halves[i]], in1.at[s, i], s1.at[s, i], r1.at[s, i], sides[i])

    def hop2(s, i):
        return remote(part.at[s, sides[i]], in2.at[s, i], s2.at[s, i], r2.at[s, i], sides[i])

    def hop3(s, i):
        return remote(norm.at[s], out_hbm.at[rows_of(me, s), :], s3.at[s, i], r3.at[s, i], sides[i])

    def hop4(s, i):
        block_rows = rows_of(sides[1 - i], s)
        where = out_hbm.at[block_rows, halves[i]]
        return remote(where, where, s4.at[s, i], r4.at[s, i], sides[i])

    def stage_a(s):
        at = pl.ds(pl.multiple_of(s * rows, rows), rows)

        def one(d, carry):
            @pl.when(s == 0)
            def _():
                w_copy(d).wait()

            left_rows = lhs[:, at, :].reshape(n_tp * rows, depth)
            prod = jnp.dot(left_rows, w[d], preferred_element_type=F32).astype(BF16)
            part[s, :, :, pl.ds(pl.multiple_of(d * n_cols, n_cols), n_cols)] = prod.reshape(n_tp, rows, n_cols)
            return carry

        lax.fori_loop(0, n_w, one, 0)
        for i in range(2):
            hop1(s, i).start()

    def stage_b(s):
        for i in range(2):
            hop1(s, i).wait_recv()
            dest = sides[i]
            mine = part[s, dest, :, halves[i]].astype(F32)
            part[s, dest, :, halves[i]] = (mine + in1[s, i].astype(F32)).astype(BF16)
            hop2(s, i).start()

    def stage_c(s):
        for i in range(2):
            hop2(s, i).wait_recv()
        step = 16

        def one(k, carry):
            at = pl.ds(pl.multiple_of(k * step, step), step)
            total = part[s, me, at, :].astype(F32) + in2[s, 0, at, :].astype(F32) + in2[s, 1, at, :].astype(F32)
            total = total.astype(BF16).astype(F32)
            res_at = pl.ds(pl.multiple_of(s * rows + k * step, step), step)
            mid = (res[res_at, :].astype(F32) + total).astype(BF16)
            if with_norm:
                own[s, at, :] = mid
                mid = mid.astype(F32)
                mean_sq = jnp.mean(mid * mid, axis=-1, keepdims=True)
                mid = (mid * lax.rsqrt(mean_sq + NORM_EPS) * gain_ref[...]).astype(BF16)
            norm[s, at, :] = mid
            return carry

        lax.fori_loop(0, rows // step, one, 0)
        for i in range(2):
            hop3(s, i).start()
        local(s).start()
        if with_norm:
            keep(s).start()

    def local(s):
        return pltpu.make_async_copy(norm.at[s], out_hbm.at[rows_of(me, s), :], o_sem.at[s, 0])

    def keep(s):
        return pltpu.make_async_copy(own.at[s], own_hbm.at[pl.ds(pl.multiple_of(s * rows, rows), rows), :], o_sem.at[s, 1])

    def arrive3(s, i):
        where = out_hbm.at[rows_of(sides[1 - i], s), :]
        return remote(norm.at[s], where, s3.at[s, i], r3.at[s, i], sides[i])

    def arrive4(s, i):
        where = out_hbm.at[rows_of(far, s), halves[i]]
        return remote(where, where, s4.at[s, i], r4.at[s, i], sides[i])

    def stage_d(s):
        for i in range(2):
            arrive3(s, i).wait_recv()
            hop4(s, i).start()

    for c in lhs_copies:
        c.wait()

    def tick(t, carry):
        @pl.when(t < N_SUB)
        def _():
            stage_a(t)

        @pl.when((t >= 1) & (t < N_SUB + 1))
        def _():
            stage_b(t - 1)

        @pl.when(t == 1)
        def _():
            for c in res_copies:
                c.wait()

        @pl.when((t >= 2) & (t < N_SUB + 2))
        def _():
            stage_c(t - 2)

        @pl.when(t >= 3)
        def _():
            stage_d(t - 3)

        return carry

    lax.fori_loop(0, N_SUB + 3, tick, 0)

    def drain(s, carry):
        local(s).wait()
        if with_norm:
            keep(s).wait()
        for i in range(2):
            hop1(s, i).wait_send()
            hop2(s, i).wait_send()
            hop3(s, i).wait_send()
            hop4(s, i).wait_send()
            arrive4(s, i).wait_recv()
        return carry

    lax.fori_loop(0, N_SUB, drain, 0)


def sum_over_tp(n_tp, lhs, w, res, gain, col_off, with_norm, collective_id, after=()):
    tokens, depth = lhs.shape
    n_w, _, n_cols = w.shape
    cols = n_w * n_cols
    block = tokens // n_tp
    rows = block // N_SUB
    out_shape = [jax.ShapeDtypeStruct((tokens, cols), BF16)]
    if with_norm:
        out_shape = [jax.ShapeDtypeStruct((block, cols), BF16)] + out_shape
    dma = pltpu.SemaphoreType.DMA
    small = (N_SUB, rows, cols) if with_norm else (1, 16, 128)
    scratch = [
        pltpu.VMEM((n_tp, block, depth), BF16),
        pltpu.VMEM((n_w, depth, n_cols), BF16),
        pltpu.VMEM((N_SUB, n_tp, rows, cols), BF16),
        pltpu.VMEM((N_SUB, 2, rows, cols // 2), BF16),
        pltpu.VMEM((N_SUB, 2, rows, cols), BF16),
        pltpu.VMEM((block, cols), BF16),
        pltpu.VMEM(small, BF16),
        pltpu.VMEM((N_SUB, rows, cols), BF16),
        dma((n_w,)), dma((n_tp,)), dma((n_w,)), dma((N_SUB, 2)),
    ] + [dma((N_SUB, 2))] * 8
    return pl.pallas_call(
        functools.partial(sum_kernel, n_tp, col_off, with_norm, len(after)),
        out_shape=out_shape,
        in_specs=[ANY, ANY, ANY, pl.BlockSpec(memory_space=pltpu.VMEM)] + [ANY] * len(after),
        out_specs=[ANY] * len(out_shape),
        scratch_shapes=scratch,
        compiler_params=pltpu.CompilerParams(collective_id=collective_id, has_side_effects=True, vmem_limit_bytes=VMEM_BIG),
        cost_estimate=pl.CostEstimate(flops=2 * tokens * cols * 30000, bytes_accessed=2 * (tokens * depth + depth * cols + 2 * tokens * cols), transcendentals=0),
        name="sum_tp_%d" % collective_id,
    )(lhs, w, res, gain, *after)


def join_kernel(n_w, a_ref, b_ref, o_ref):
    wa, wb = a_ref.shape[1] // n_w, b_ref.shape[1] // n_w
    for d in range(n_w):
        base = d * (wa + wb)
        o_ref[:, base:base + wa] = a_ref[:, d * wa:(d + 1) * wa]
        o_ref[:, base + wa:base + wa + wb] = b_ref[:, d * wb:(d + 1) * wb]


def join_columns(a, b, n_w):
    tokens = a.shape[0]
    rows = min(256, tokens)
    cols = a.shape[1] + b.shape[1]
    return pl.pallas_call(
        functools.partial(join_kernel, n_w),
        grid=(tokens // rows,),
        out_shape=jax.ShapeDtypeStruct((tokens, cols), BF16),
        in_specs=[pl.BlockSpec((rows, a.shape[1]), lambda i: (i, 0)), pl.BlockSpec((rows, b.shape[1]), lambda i: (i, 0))],
        out_specs=pl.BlockSpec((rows, cols), lambda i: (i, 0)),
        cost_estimate=pl.CostEstimate(flops=tokens * cols, bytes_accessed=4 * tokens * cols, transcendentals=0),
        name="join",
    )(a, b)


def solution(mesh):
    seq_spec = P(('dp', 'fsdp'), 'cp', None)
    pos_spec = P(('dp', 'fsdp'), 'cp')
    in_spec = P(GROUP_AXES, 'tp', None)
    out_spec = P('tp', None, GROUP_AXES)
    col_spec = P(GROUP_AXES, 'tp')
    row_spec = P('tp', GROUP_AXES)
    rep_spec = P(None)
    n_tp = mesh.shape['tp']
    n_w = mesh.shape['fsdp'] * mesh.shape['cp']

    def layer_local(hidden, positions, attn_gain, w_query, w_key, w_value, w_out, mlp_gain, w_gate, w_up, w_down):
        tokens, d_model = hidden.shape[1:]
        share, heads, head_dim = w_query.shape
        kv_heads = w_key.shape[1]
        w_qkv = jnp.concatenate([w.reshape(share, -1) for w in (w_query, w_key, w_value)], axis=1)
        full_qkv = lax.all_gather(w_qkv, GROUP_AXES, axis=0, tiled=True)
        full_out = lax.all_gather(w_out.reshape(heads * head_dim, share), GROUP_AXES, axis=0, tiled=False)
        full_gate = lax.all_gather(w_gate, GROUP_AXES, axis=0, tiled=True)
        full_up = lax.all_gather(w_up, GROUP_AXES, axis=0, tiled=True)
        cut = (share * 2 // 5) // 128 * 128
        full_down0 = lax.all_gather(w_down[:, :cut], GROUP_AXES, axis=0, tiled=False)
        full_down1 = lax.all_gather(w_down[:, cut:], GROUP_AXES, axis=0, tiled=False)

        x = hidden[0]
        normed = rms_norm(x.astype(F32), attn_gain)
        cos, sin = rope_tables(positions[0], head_dim)
        qkv = project_qkv(normed, full_qkv, cos, sin, heads + kv_heads)
        kv = qkv[:, heads * head_dim:]
        kv_peer = lax.ppermute(kv, 'cp', [(0, 1), (1, 0)])
        c = lax.axis_index('cp')
        table = jnp.where(c == 0, jnp.array([0, 2, 3, 1, 0, 3], jnp.int32), jnp.array([2, 0, 1, 3, 1, 2], jnp.int32))
        kv_all = jnp.concatenate([kv, kv_peer], axis=0)
        k_all, vt_all = kv_all[:, :kv_heads * head_dim], kv_all[:, kv_heads * head_dim:].T
        mixed = attention(qkv, k_all, vt_all, table, heads, kv_heads, head_dim)
        mid_own, normed_mlp = sum_over_tp(n_tp, mixed, full_out, x, attn_gain_row(mlp_gain), 0, True, 0)
        gate_proj = jnp.dot(normed_mlp, full_gate, preferred_element_type=F32)
        up_proj = jnp.dot(normed_mlp, full_up, preferred_element_type=F32)
        act = (jax.nn.silu(gate_proj) * up_proj).astype(BF16)
        piece0, = sum_over_tp(n_tp, act, full_down0, mid_own, attn_gain_row(mlp_gain), 0, False, 1)
        piece1, = sum_over_tp(n_tp, act, full_down1, mid_own, attn_gain_row(mlp_gain), cut, False, 2, after=(piece0,))
        return join_columns(piece0, piece1, n_w)[None]

    return jax.shard_map(layer_local, mesh=mesh, in_specs=(seq_spec, pos_spec, rep_spec, in_spec, in_spec, in_spec, out_spec, rep_spec, col_spec, col_spec, row_spec), out_specs=seq_spec, check_vma=False)


def attn_gain_row(gain):
    return gain[None, :]
```

```python
import functools

import jax
import jax.numpy as jnp
from jax import lax
from jax.experimental import pallas as pl
from jax.experimental.pallas import tpu as pltpu
from jax.sharding import PartitionSpec as P

ROPE_THETA = 500000.0
NORM_EPS = 1e-5
GROUP_AXES = ('fsdp', 'cp')
N_SUB = 6
F32 = jnp.float32
BF16 = jnp.bfloat16
MESH = pl.DeviceIdType.MESH
VMEM_BIG = 58 * 1024 * 1024
ANY = pl.BlockSpec(memory_space=pl.ANY)


def rms_norm(hidden_f32, gain):
    mean_sq = jnp.mean(hidden_f32 * hidden_f32, axis=-1, keepdims=True)
    return (hidden_f32 * lax.rsqrt(mean_sq + NORM_EPS) * gain).astype(BF16)


def rope_tables(positions, head_dim):
    inv_freq = ROPE_THETA ** (-jnp.arange(0, head_dim, 2, dtype=F32) / head_dim)
    angles = positions.astype(F32)[..., None] * inv_freq
    cos, sin = jnp.cos(angles), jnp.sin(angles)
    return jnp.concatenate([cos, cos], axis=-1), jnp.concatenate([-sin, sin], axis=-1)


def qkv_kernel(head_dim, rope_heads, a_ref, w_ref, cos_ref, sin_ref, o_ref):
    cols = w_ref.shape[1]
    step = 4 * head_dim
    cos, sin = cos_ref[...], sin_ref[...]
    for start in range(0, cols, step):
        proj = jnp.dot(a_ref[...], w_ref[:, start:start + step], preferred_element_type=F32)
        for k in range(step // head_dim):
            x = proj[:, k * head_dim:(k + 1) * head_dim]
            if start // head_dim + k < rope_heads:
                x = x * cos + pltpu.roll(x, head_dim // 2, 1) * sin
            o_ref[:, start + k * head_dim:start + (k + 1) * head_dim] = x.astype(BF16)


def project_qkv(a, w, cos, sin, rope_heads):
    tokens, d_model = a.shape
    cols, head_dim = w.shape[1], cos.shape[1]
    rows = min(256, tokens)
    return pl.pallas_call(
        functools.partial(qkv_kernel, head_dim, rope_heads),
        grid=(tokens // rows,),
        out_shape=jax.ShapeDtypeStruct((tokens, cols), BF16),
        in_specs=[
            pl.BlockSpec((rows, d_model), lambda i: (i, 0)),
            pl.BlockSpec((d_model, cols), lambda i: (0, 0), pipeline_mode=pl.Buffered(1)),
            pl.BlockSpec((rows, head_dim), lambda i: (i, 0)),
            pl.BlockSpec((rows, head_dim), lambda i: (i, 0)),
        ],
        out_specs=pl.BlockSpec((rows, cols), lambda i: (i, 0)),
        compiler_params=pltpu.CompilerParams(vmem_limit_bytes=VMEM_BIG),
        cost_estimate=pl.CostEstimate(flops=2 * tokens * d_model * cols, bytes_accessed=2 * (tokens * d_model + d_model * cols + tokens * cols), transcendentals=0),
        name="qkv",
    )(a, w, cos, sin)


def attn_kernel(group, head_dim, per_seg, table_ref, q_ref, k_ref, vt_ref, o_ref, m_sc, l_sc, acc_sc):
    blk = q_ref.shape[0]
    seg_rows = per_seg * blk
    qi = pl.program_id(1)
    true_seg = table_ref[4 + qi // per_seg]
    scale = (head_dim ** -0.5) * 1.4426950408889634
    m_sc[...] = jnp.full(m_sc.shape, -1e30, F32)
    l_sc[...] = jnp.zeros(l_sc.shape, F32)
    acc_sc[...] = jnp.zeros(acc_sc.shape, F32)

    def step(j, n_keys, within):
        rows = pl.ds(pl.multiple_of(table_ref[j] * seg_rows, seg_rows), n_keys)
        k, vt = k_ref[rows, :], vt_ref[:, rows]
        for h in range(group):
            q = q_ref[:, h * head_dim:(h + 1) * head_dim]
            s = lax.dot_general(k, q, (((1,), (1,)), ((), ())), preferred_element_type=F32) * scale
            if within is not None:
                keep = lax.broadcasted_iota(jnp.int32, s.shape, 0) <= lax.broadcasted_iota(jnp.int32, s.shape, 1) + within
                s = jnp.where(keep, s, -1e30)
            m_old = m_sc[h]
            m_new = jnp.maximum(m_old, jnp.max(s, axis=0, keepdims=True))
            alpha = jnp.exp2(m_old - m_new)
            p = jnp.exp2(s - m_new)
            l_sc[h] = l_sc[h] * alpha + jnp.sum(p, axis=0, keepdims=True)
            acc_sc[h] = acc_sc[h] * alpha + jnp.dot(vt, p.astype(BF16), preferred_element_type=F32)
            m_sc[h] = m_new

    def body(j, carry):
        step(j, seg_rows, None)
        return carry

    lax.fori_loop(0, true_seg, body, 0)
    for w in range(per_seg):
        @pl.when(lax.rem(qi, per_seg) == w)
        def _():
            step(true_seg, (w + 1) * blk, w * blk)

    for h in range(group):
        o_ref[:, h * head_dim:(h + 1) * head_dim] = (acc_sc[h] / l_sc[h]).T.astype(BF16)


def attention(qkv, k_all, vt_all, table, heads, kv_heads, head_dim):
    tokens, keys = qkv.shape[0], k_all.shape[0]
    seg_rows = tokens // 2
    blk = min(256, seg_rows)
    per_seg = seg_rows // blk
    group = heads // kv_heads
    return pl.pallas_call(
        functools.partial(attn_kernel, group, head_dim, per_seg),
        grid_spec=pltpu.PrefetchScalarGridSpec(
            num_scalar_prefetch=1,
            grid=(kv_heads, tokens // blk),
            in_specs=[
                pl.BlockSpec((blk, group * head_dim), lambda g, i, t: (i, g)),
                pl.BlockSpec((keys, head_dim), lambda g, i, t: (0, g)),
                pl.BlockSpec((head_dim, keys), lambda g, i, t: (g, 0)),
            ],
            out_specs=pl.BlockSpec((blk, group * head_dim), lambda g, i, t: (i, g)),
            scratch_shapes=[pltpu.VMEM((group, 1, blk), F32), pltpu.VMEM((group, 1, blk), F32), pltpu.VMEM((group, head_dim, blk), F32)],
        ),
        out_shape=jax.ShapeDtypeStruct((tokens, heads * head_dim), BF16),
        compiler_params=pltpu.CompilerParams(vmem_limit_bytes=32 * 1024 * 1024),
        cost_estimate=pl.CostEstimate(flops=2 * tokens * keys * heads * head_dim * 2, bytes_accessed=2 * (2 * tokens * heads * head_dim + 4 * keys * head_dim), transcendentals=tokens * keys * heads),
        name="attn",
    )(table, qkv, k_all, vt_all)


def sum_kernel(n_tp, col_off, with_norm, n_after, lhs_hbm, w_hbm, res_hbm, gain_ref, *refs):
    refs = refs[n_after:]
    if with_norm:
        own_hbm, out_hbm = refs[:2]
        refs = refs[2:]
    else:
        out_hbm = refs[0]
        refs = refs[1:]
    lhs, w, part, in1, in2, res, own, norm, w_sem, l_sem, r_sem, o_sem, s1, r1, s2, r2, s3, r3, s4, r4 = refs
    n_w, depth, n_cols = w.shape
    cols = n_w * n_cols
    half = cols // 2
    rows = part.shape[2]
    block = rows * N_SUB
    me = lax.axis_index("tp")
    right, left = lax.rem(me + 1, n_tp), lax.rem(me + n_tp - 1, n_tp)
    far = lax.rem(me + 2, n_tp)
    sides = (right, left)
    lo, hi = pl.ds(0, half), pl.ds(half, half)
    halves = (lo, hi)

    def w_copy(d):
        return pltpu.make_async_copy(w_hbm.at[d], w.at[d], w_sem.at[d])

    lhs_copies = [pltpu.make_async_copy(lhs_hbm.at[pl.ds(b * block, block), :], lhs.at[b], l_sem.at[b]) for b in range(n_tp)]
    for c in lhs_copies:
        c.start()
    for d in range(n_w):
        w_copy(d).start()
    my_rows = pl.ds(pl.multiple_of(me * block, block), block)
    if with_norm:
        res_copies = [pltpu.make_async_copy(res_hbm.at[my_rows, :], res, r_sem.at[0])]
    else:
        wide = res_hbm.shape[1] // n_w
        res_copies = [pltpu.make_async_copy(res_hbm.at[:, pl.ds(d * wide + col_off, n_cols)], res.at[:, pl.ds(d * n_cols, n_cols)], r_sem.at[d]) for d in range(n_w)]
    for c in res_copies:
        c.start()

    barrier = pltpu.get_barrier_semaphore()
    for dev in sides:
        pl.semaphore_signal(barrier, inc=1, device_id={"tp": dev}, device_id_type=MESH)
    pl.semaphore_wait(barrier, 2)

    def remote(src, dst, send, recv, dev):
        return pltpu.make_async_remote_copy(src_ref=src, dst_ref=dst, send_sem=send, recv_sem=recv, device_id={"tp": dev}, device_id_type=MESH)

    def rows_of(b, s):
        return pl.ds(pl.multiple_of(b * block + s * rows, rows), rows)

    def hop1(s, i):
        return remote(part.at[s, far, :, halves[i]], in1.at[s, i], s1.at[s, i], r1.at[s, i], sides[i])

    def hop2(s, i):
        return remote(part.at[s, sides[i]], in2.at[s, i], s2.at[s, i], r2.at[s, i], sides[i])

    def hop3(s, i):
        return remote(norm.at[s], out_hbm.at[rows_of(me, s), :], s3.at[s, i], r3.at[s, i], sides[i])

    def hop4(s, i):
        block_rows = rows_of(sides[1 - i], s)
        where = out_hbm.at[block_rows, halves[i]]
        return remote(where, where, s4.at[s, i], r4.at[s, i], sides[i])

    def stage_a(s):
        at = pl.ds(pl.multiple_of(s * rows, rows), rows)

        def one(d, carry):
            @pl.when(s == 0)
            def _():
                w_copy(d).wait()

            left_rows = lhs[:, at, :].reshape(n_tp * rows, depth)
            prod = jnp.dot(left_rows, w[d], preferred_element_type=F32).astype(BF16)
            part[s, :, :, pl.ds(pl.multiple_of(d * n_cols, n_cols), n_cols)] = prod.reshape(n_tp, rows, n_cols)
            return carry

        lax.fori_loop(0, n_w, one, 0)
        for i in range(2):
            hop1(s, i).start()

    def stage_b(s):
        for i in range(2):
            hop1(s, i).wait_recv()
            dest = sides[i]
            mine = part[s, dest, :, halves[i]].astype(F32)
            part[s, dest, :, halves[i]] = (mine + in1[s, i].astype(F32)).astype(BF16)
            hop2(s, i).start()

    def stage_c(s):
        for i in range(2):
            hop2(s, i).wait_recv()
        step = 16

        def one(k, carry):
            at = pl.ds(pl.multiple_of(k * step, step), step)
            total = part[s, me, at, :].astype(F32) + in2[s, 0, at, :].astype(F32) + in2[s, 1, at, :].astype(F32)
            total = total.astype(BF16).astype(F32)
            res_at = pl.ds(pl.multiple_of(s * rows + k * step, step), step)
            mid = (res[res_at, :].astype(F32) + total).astype(BF16)
            if with_norm:
                own[s, at, :] = mid
                mid = mid.astype(F32)
                mean_sq = jnp.mean(mid * mid, axis=-1, keepdims=True)
                mid = (mid * lax.rsqrt(mean_sq + NORM_EPS) * gain_ref[...]).astype(BF16)
            norm[s, at, :] = mid
            return carry

        lax.fori_loop(0, rows // step, one, 0)
        if not with_norm:
            for i in range(2):
                hop3(s, i).start()
        local(s).start()
        if with_norm:
            keep(s).start()

    def local(s):
        where = pl.ds(pl.multiple_of(s * rows, rows), rows) if with_norm else rows_of(me, s)
        return pltpu.make_async_copy(norm.at[s], out_hbm.at[where, :], o_sem.at[s, 0])

    def keep(s):
        return pltpu.make_async_copy(own.at[s], own_hbm.at[pl.ds(pl.multiple_of(s * rows, rows), rows), :], o_sem.at[s, 1])

    def arrive3(s, i):
        where = out_hbm.at[rows_of(sides[1 - i], s), :]
        return remote(norm.at[s], where, s3.at[s, i], r3.at[s, i], sides[i])

    def arrive4(s, i):
        where = out_hbm.at[rows_of(far, s), halves[i]]
        return remote(where, where, s4.at[s, i], r4.at[s, i], sides[i])

    def stage_d(s):
        for i in range(2):
            arrive3(s, i).wait_recv()
            hop4(s, i).start()

    for c in lhs_copies:
        c.wait()

    def tick(t, carry):
        @pl.when(t < N_SUB)
        def _():
            stage_a(t)

        @pl.when((t >= 1) & (t < N_SUB + 1))
        def _():
            stage_b(t - 1)

        @pl.when(t == 1)
        def _():
            for c in res_copies:
                c.wait()

        @pl.when((t >= 2) & (t < N_SUB + 2))
        def _():
            stage_c(t - 2)

        if not with_norm:
            @pl.when(t >= 3)
            def _():
                stage_d(t - 3)

        return carry

    lax.fori_loop(0, N_SUB + (2 if with_norm else 3), tick, 0)

    def drain(s, carry):
        local(s).wait()
        if with_norm:
            keep(s).wait()
        for i in range(2):
            hop1(s, i).wait_send()
            hop2(s, i).wait_send()
            if not with_norm:
                hop3(s, i).wait_send()
                hop4(s, i).wait_send()
                arrive4(s, i).wait_recv()
        return carry

    lax.fori_loop(0, N_SUB, drain, 0)


def sum_over_tp(n_tp, lhs, w, res, gain, col_off, with_norm, collective_id, after=()):
    tokens, depth = lhs.shape
    n_w, _, n_cols = w.shape
    cols = n_w * n_cols
    block = tokens // n_tp
    rows = block // N_SUB
    out_shape = [jax.ShapeDtypeStruct((block, cols), BF16)] * 2 if with_norm else [jax.ShapeDtypeStruct((tokens, cols), BF16)]
    dma = pltpu.SemaphoreType.DMA
    small = (N_SUB, rows, cols) if with_norm else (1, 16, 128)
    scratch = [
        pltpu.VMEM((n_tp, block, depth), BF16),
        pltpu.VMEM((n_w, depth, n_cols), BF16),
        pltpu.VMEM((N_SUB, n_tp, rows, cols), BF16),
        pltpu.VMEM((N_SUB, 2, rows, cols // 2), BF16),
        pltpu.VMEM((N_SUB, 2, rows, cols), BF16),
        pltpu.VMEM((block, cols), BF16),
        pltpu.VMEM(small, BF16),
        pltpu.VMEM((N_SUB, rows, cols), BF16),
        dma((n_w,)), dma((n_tp,)), dma((n_w,)), dma((N_SUB, 2)),
    ] + [dma((N_SUB, 2))] * 8
    return pl.pallas_call(
        functools.partial(sum_kernel, n_tp, col_off, with_norm, len(after)),
        out_shape=out_shape,
        in_specs=[ANY, ANY, ANY, pl.BlockSpec(memory_space=pltpu.VMEM)] + [ANY] * len(after),
        out_specs=[ANY] * len(out_shape),
        scratch_shapes=scratch,
        compiler_params=pltpu.CompilerParams(collective_id=collective_id, has_side_effects=True, vmem_limit_bytes=VMEM_BIG),
        cost_estimate=pl.CostEstimate(flops=2 * tokens * cols * 30000, bytes_accessed=2 * (tokens * depth + depth * cols + 2 * tokens * cols), transcendentals=0),
        name="sum_tp_%d" % collective_id,
    )(lhs, w, res, gain, *after)


def gate_kernel(n_tp, own_hbm, w_hbm, all_hbm, gate_hbm, w, xs, ys, w_sem, x_sem, y_sem, l_sem, s1, r1, s2, r2):
    block, depth = own_hbm.shape
    part = block // 2
    half = depth // 2
    cols = w.shape[1]
    n_chunks = w_sem.shape[0]
    chunk = cols // n_chunks
    me = lax.axis_index("tp")
    right, left = lax.rem(me + 1, n_tp), lax.rem(me + n_tp - 1, n_tp)
    far = lax.rem(me + 2, n_tp)
    sides = (right, left)
    halves = (pl.ds(0, half), pl.ds(half, half))

    def rows_of(b, p):
        return pl.ds(pl.multiple_of(b * block + p * part, part), part)

    def part_of(p):
        return pl.ds(pl.multiple_of(p * part, part), part)

    def w_copy(n):
        at = pl.ds(pl.multiple_of(n * chunk, chunk), chunk)
        return pltpu.make_async_copy(w_hbm.at[:, at], w.at[:, at], w_sem.at[n])

    def remote(src, dst, send, recv, dev):
        return pltpu.make_async_remote_copy(src_ref=src, dst_ref=dst, send_sem=send, recv_sem=recv, device_id={"tp": dev}, device_id_type=MESH)

    def hop1(p, i):
        return remote(own_hbm.at[part_of(p), :], all_hbm.at[rows_of(me, p), :], s1.at[p, i], r1.at[p, i], sides[i])

    def hop2(p, i):
        where = all_hbm.at[rows_of(sides[1 - i], p), halves[i]]
        return remote(where, where, s2.at[p, i], r2.at[p, i], sides[i])

    def arrive1(p, i):
        where = all_hbm.at[rows_of(sides[1 - i], p), :]
        return remote(own_hbm.at[part_of(p), :], where, s1.at[p, i], r1.at[p, i], sides[i])

    def arrive2(p, i):
        where = all_hbm.at[rows_of(far, p), halves[i]]
        return remote(where, where, s2.at[p, i], r2.at[p, i], sides[i])

    def y_copy(k, rows):
        return pltpu.make_async_copy(ys.at[part_of(k)], gate_hbm.at[rows, :], y_sem.at[k])

    barrier = pltpu.get_barrier_semaphore()
    for dev in sides:
        pl.semaphore_signal(barrier, inc=1, device_id={"tp": dev}, device_id_type=MESH)
    pl.semaphore_wait(barrier, 2)
    for p in range(2):
        for i in range(2):
            hop1(p, i).start()
    own_copies = [pltpu.make_async_copy(own_hbm.at[part_of(p), :], xs.at[part_of(p)], x_sem.at[p]) for p in range(2)]
    for c in own_copies:
        c.start()
    for n in range(n_chunks):
        w_copy(n).start()
    for c in own_copies:
        c.wait()
    local_copies = [pltpu.make_async_copy(xs.at[part_of(p)], all_hbm.at[rows_of(me, p), :], l_sem.at[p]) for p in range(2)]
    for c in local_copies:
        c.start()

    def unit(u, carry):
        p = jnp.maximum(u - 1, 0)
        where = [rows_of(jnp.where(u == 0, me, sides[1 - k]), jnp.where(u == 0, k, p)) for k in range(2)]

        @pl.when(u >= 1)
        def _():
            for i in range(2):
                arrive1(p, i).wait_recv()
                hop2(p, i).start()

            @pl.when(u == 1)
            def _():
                for c in local_copies:
                    c.wait()

            loads = [pltpu.make_async_copy(all_hbm.at[where[k], :], xs.at[part_of(k)], x_sem.at[k]) for k in range(2)]
            for c in loads:
                c.start()
            for k in range(2):
                y_copy(k, where[k]).wait()
            for c in loads:
                c.wait()

        def one(n, c):
            at = pl.ds(pl.multiple_of(n * chunk, chunk), chunk)

            @pl.when(u == 0)
            def _():
                w_copy(n).wait()

            ys[:, at] = jnp.dot(xs[...], w[:, at], preferred_element_type=F32)
            return c

        lax.fori_loop(0, n_chunks, one, 0)
        for k in range(2):
            y_copy(k, where[k]).start()
        return carry

    lax.fori_loop(0, 3, unit, 0)
    y_copy(0, rows_of(far, 0)).wait()
    y_copy(1, rows_of(far, 1)).wait()

    def last(p, carry):
        for i in range(2):
            arrive2(p, i).wait_recv()
        load = pltpu.make_async_copy(all_hbm.at[rows_of(far, p), :], xs.at[part_of(p)], x_sem.at[p])
        load.start()
        load.wait()

        def one(n, c):
            at = pl.ds(pl.multiple_of(n * chunk, chunk), chunk)
            ys[part_of(p), at] = jnp.dot(xs[part_of(p), :], w[:, at], preferred_element_type=F32)
            return c

        lax.fori_loop(0, n_chunks, one, 0)
        y_copy(p, rows_of(far, p)).start()
        return carry

    lax.fori_loop(0, 2, last, 0)
    for p in range(2):
        y_copy(p, rows_of(far, p)).wait()
        for i in range(2):
            hop1(p, i).wait_send()
            hop2(p, i).wait_send()


def gather_and_gate(n_tp, own, w, collective_id):
    block, depth = own.shape
    cols = w.shape[1]
    tokens = n_tp * block
    chunk = next(c for c in (512, 256, 128) if cols % c == 0)
    dma = pltpu.SemaphoreType.DMA
    return pl.pallas_call(
        functools.partial(gate_kernel, n_tp),
        out_shape=[jax.ShapeDtypeStruct((tokens, depth), BF16), jax.ShapeDtypeStruct((tokens, cols), F32)],
        in_specs=[ANY, ANY],
        out_specs=[ANY, ANY],
        scratch_shapes=[
            pltpu.VMEM((depth, cols), BF16), pltpu.VMEM((block, depth), BF16), pltpu.VMEM((block, cols), F32),
            dma((cols // chunk,)), dma((2,)), dma((2,)), dma((2,)),
        ] + [dma((2, 2))] * 4,
        compiler_params=pltpu.CompilerParams(collective_id=collective_id, has_side_effects=True, vmem_limit_bytes=VMEM_BIG),
        cost_estimate=pl.CostEstimate(flops=2 * tokens * cols * depth * 3, bytes_accessed=2 * (tokens * depth + depth * cols + 2 * tokens * cols), transcendentals=0),
        name="gather_gate",
    )(own, w)


def join_kernel(n_w, a_ref, b_ref, o_ref):
    wa, wb = a_ref.shape[1] // n_w, b_ref.shape[1] // n_w
    for d in range(n_w):
        base = d * (wa + wb)
        o_ref[:, base:base + wa] = a_ref[:, d * wa:(d + 1) * wa]
        o_ref[:, base + wa:base + wa + wb] = b_ref[:, d * wb:(d + 1) * wb]


def join_columns(a, b, n_w):
    tokens = a.shape[0]
    rows = min(256, tokens)
    cols = a.shape[1] + b.shape[1]
    return pl.pallas_call(
        functools.partial(join_kernel, n_w),
        grid=(tokens // rows,),
        out_shape=jax.ShapeDtypeStruct((tokens, cols), BF16),
        in_specs=[pl.BlockSpec((rows, a.shape[1]), lambda i: (i, 0)), pl.BlockSpec((rows, b.shape[1]), lambda i: (i, 0))],
        out_specs=pl.BlockSpec((rows, cols), lambda i: (i, 0)),
        cost_estimate=pl.CostEstimate(flops=tokens * cols, bytes_accessed=4 * tokens * cols, transcendentals=0),
        name="join",
    )(a, b)


def solution(mesh):
    seq_spec = P(('dp', 'fsdp'), 'cp', None)
    pos_spec = P(('dp', 'fsdp'), 'cp')
    in_spec = P(GROUP_AXES, 'tp', None)
    out_spec = P('tp', None, GROUP_AXES)
    col_spec = P(GROUP_AXES, 'tp')
    row_spec = P('tp', GROUP_AXES)
    rep_spec = P(None)
    n_tp = mesh.shape['tp']
    n_w = mesh.shape['fsdp'] * mesh.shape['cp']

    def layer_local(hidden, positions, attn_gain, w_query, w_key, w_value, w_out, mlp_gain, w_gate, w_up, w_down):
        tokens, d_model = hidden.shape[1:]
        share, heads, head_dim = w_query.shape
        kv_heads = w_key.shape[1]
        w_qkv = jnp.concatenate([w.reshape(share, -1) for w in (w_query, w_key, w_value)], axis=1)
        full_qkv = lax.all_gather(w_qkv, GROUP_AXES, axis=0, tiled=True)
        full_out = lax.all_gather(w_out.reshape(heads * head_dim, share), GROUP_AXES, axis=0, tiled=False)
        full_gate = lax.all_gather(w_gate, GROUP_AXES, axis=0, tiled=True)
        full_up = lax.all_gather(w_up, GROUP_AXES, axis=0, tiled=True)
        cut = (share * 2 // 5) // 128 * 128
        x = hidden[0]
        normed = rms_norm(x.astype(F32), attn_gain)
        down0, down1, normed = lax.optimization_barrier((w_down[:, :cut], w_down[:, cut:], normed))
        full_down0 = lax.all_gather(down0, GROUP_AXES, axis=0, tiled=False)
        full_down1 = lax.all_gather(down1, GROUP_AXES, axis=0, tiled=False)
        cos, sin = rope_tables(positions[0], head_dim)
        qkv = project_qkv(normed, full_qkv, cos, sin, heads + kv_heads)
        kv = qkv[:, heads * head_dim:]
        kv_peer = lax.ppermute(kv, 'cp', [(0, 1), (1, 0)])
        c = lax.axis_index('cp')
        table = jnp.where(c == 0, jnp.array([0, 2, 3, 1, 0, 3], jnp.int32), jnp.array([2, 0, 1, 3, 1, 2], jnp.int32))
        kv_all = jnp.concatenate([kv, kv_peer], axis=0)
        k_all, vt_all = kv_all[:, :kv_heads * head_dim], kv_all[:, kv_heads * head_dim:].T
        mixed = attention(qkv, k_all, vt_all, table, heads, kv_heads, head_dim)
        mid_own, normed_own = sum_over_tp(n_tp, mixed, full_out, x, attn_gain_row(mlp_gain), 0, True, 0)
        normed_mlp, gate_proj = gather_and_gate(n_tp, normed_own, full_gate, 3)
        up_proj = jnp.dot(normed_mlp, full_up, preferred_element_type=F32)
        act = (jax.nn.silu(gate_proj) * up_proj).astype(BF16)
        piece0, = sum_over_tp(n_tp, act, full_down0, mid_own, attn_gain_row(mlp_gain), 0, False, 1)
        piece1, = sum_over_tp(n_tp, act, full_down1, mid_own, attn_gain_row(mlp_gain), cut, False, 2, after=(piece0,))
        return join_columns(piece0, piece1, n_w)[None]

    return jax.shard_map(layer_local, mesh=mesh, in_specs=(seq_spec, pos_spec, rep_spec, in_spec, in_spec, in_spec, out_spec, rep_spec, col_spec, col_spec, row_spec), out_specs=seq_spec, check_vma=False)


def attn_gain_row(gain):
    return gain[None, :]
```

```python
import functools

import jax
import jax.numpy as jnp
from jax import lax
from jax.experimental import pallas as pl
from jax.experimental.pallas import tpu as pltpu
from jax.sharding import PartitionSpec as P

ROPE_THETA = 500000.0
NORM_EPS = 1e-5
GROUP_AXES = ('fsdp', 'cp')
N_SUB = 8
F32 = jnp.float32
BF16 = jnp.bfloat16
MESH = pl.DeviceIdType.MESH
VMEM_BIG = 58 * 1024 * 1024
ANY = pl.BlockSpec(memory_space=pl.ANY)


def rms_norm(hidden_f32, gain):
    mean_sq = jnp.mean(hidden_f32 * hidden_f32, axis=-1, keepdims=True)
    return (hidden_f32 * lax.rsqrt(mean_sq + NORM_EPS) * gain).astype(BF16)


def rope_tables(positions, head_dim):
    inv_freq = ROPE_THETA ** (-jnp.arange(0, head_dim, 2, dtype=F32) / head_dim)
    angles = positions.astype(F32)[..., None] * inv_freq
    cos, sin = jnp.cos(angles), jnp.sin(angles)
    return jnp.concatenate([cos, cos], axis=-1), jnp.concatenate([-sin, sin], axis=-1)


def qkv_kernel(head_dim, rope_heads, a_ref, w_ref, cos_ref, sin_ref, o_ref):
    cols = w_ref.shape[1]
    step = 4 * head_dim
    cos, sin = cos_ref[...], sin_ref[...]
    for start in range(0, cols, step):
        proj = jnp.dot(a_ref[...], w_ref[:, start:start + step], preferred_element_type=F32)
        for k in range(step // head_dim):
            x = proj[:, k * head_dim:(k + 1) * head_dim]
            if start // head_dim + k < rope_heads:
                x = x * cos + pltpu.roll(x, head_dim // 2, 1) * sin
            o_ref[:, start + k * head_dim:start + (k + 1) * head_dim] = x.astype(BF16)


def project_qkv(a, w, cos, sin, rope_heads):
    tokens, d_model = a.shape
    cols, head_dim = w.shape[1], cos.shape[1]
    rows = min(256, tokens)
    return pl.pallas_call(
        functools.partial(qkv_kernel, head_dim, rope_heads),
        grid=(tokens // rows,),
        out_shape=jax.ShapeDtypeStruct((tokens, cols), BF16),
        in_specs=[
            pl.BlockSpec((rows, d_model), lambda i: (i, 0)),
            pl.BlockSpec((d_model, cols), lambda i: (0, 0), pipeline_mode=pl.Buffered(1)),
            pl.BlockSpec((rows, head_dim), lambda i: (i, 0)),
            pl.BlockSpec((rows, head_dim), lambda i: (i, 0)),
        ],
        out_specs=pl.BlockSpec((rows, cols), lambda i: (i, 0)),
        compiler_params=pltpu.CompilerParams(vmem_limit_bytes=VMEM_BIG),
        cost_estimate=pl.CostEstimate(flops=2 * tokens * d_model * cols, bytes_accessed=2 * (tokens * d_model + d_model * cols + tokens * cols), transcendentals=0),
        name="qkv",
    )(a, w, cos, sin)


def attn_kernel(group, head_dim, per_seg, table_ref, q_ref, k_ref, vt_ref, o_ref, m_sc, l_sc, acc_sc):
    blk = q_ref.shape[0]
    seg_rows = per_seg * blk
    qi = pl.program_id(1)
    true_seg = table_ref[4 + qi // per_seg]
    scale = (head_dim ** -0.5) * 1.4426950408889634
    m_sc[...] = jnp.full(m_sc.shape, -1e30, F32)
    l_sc[...] = jnp.zeros(l_sc.shape, F32)
    acc_sc[...] = jnp.zeros(acc_sc.shape, F32)

    def step(j, n_keys, within):
        rows = pl.ds(pl.multiple_of(table_ref[j] * seg_rows, seg_rows), n_keys)
        k, vt = k_ref[rows, :], vt_ref[:, rows]
        for h in range(group):
            q = q_ref[:, h * head_dim:(h + 1) * head_dim]
            s = lax.dot_general(k, q, (((1,), (1,)), ((), ())), preferred_element_type=F32) * scale
            if within is not None:
                keep = lax.broadcasted_iota(jnp.int32, s.shape, 0) <= lax.broadcasted_iota(jnp.int32, s.shape, 1) + within
                s = jnp.where(keep, s, -1e30)
            m_old = m_sc[h]
            m_new = jnp.maximum(m_old, jnp.max(s, axis=0, keepdims=True))
            alpha = jnp.exp2(m_old - m_new)
            p = jnp.exp2(s - m_new)
            l_sc[h] = l_sc[h] * alpha + jnp.sum(p, axis=0, keepdims=True)
            acc_sc[h] = acc_sc[h] * alpha + jnp.dot(vt, p.astype(BF16), preferred_element_type=F32)
            m_sc[h] = m_new

    def body(j, carry):
        step(j, seg_rows, None)
        return carry

    lax.fori_loop(0, true_seg, body, 0)
    for w in range(per_seg):
        @pl.when(lax.rem(qi, per_seg) == w)
        def _():
            step(true_seg, (w + 1) * blk, w * blk)

    for h in range(group):
        o_ref[:, h * head_dim:(h + 1) * head_dim] = (acc_sc[h] / l_sc[h]).T.astype(BF16)


def attention(qkv, k_all, vt_all, table, heads, kv_heads, head_dim):
    tokens, keys = qkv.shape[0], k_all.shape[0]
    seg_rows = tokens // 2
    blk = min(256, seg_rows)
    per_seg = seg_rows // blk
    group = heads // kv_heads
    return pl.pallas_call(
        functools.partial(attn_kernel, group, head_dim, per_seg),
        grid_spec=pltpu.PrefetchScalarGridSpec(
            num_scalar_prefetch=1,
            grid=(kv_heads, tokens // blk),
            in_specs=[
                pl.BlockSpec((blk, group * head_dim), lambda g, i, t: (i, g)),
                pl.BlockSpec((keys, head_dim), lambda g, i, t: (0, g)),
                pl.BlockSpec((head_dim, keys), lambda g, i, t: (g, 0)),
            ],
            out_specs=pl.BlockSpec((blk, group * head_dim), lambda g, i, t: (i, g)),
            scratch_shapes=[pltpu.VMEM((group, 1, blk), F32), pltpu.VMEM((group, 1, blk), F32), pltpu.VMEM((group, head_dim, blk), F32)],
        ),
        out_shape=jax.ShapeDtypeStruct((tokens, heads * head_dim), BF16),
        compiler_params=pltpu.CompilerParams(vmem_limit_bytes=32 * 1024 * 1024),
        cost_estimate=pl.CostEstimate(flops=2 * tokens * keys * heads * head_dim * 2, bytes_accessed=2 * (2 * tokens * heads * head_dim + 4 * keys * head_dim), transcendentals=tokens * keys * heads),
        name="attn",
    )(table, qkv, k_all, vt_all)


def sum_kernel(n_tp, col_off, with_norm, n_after, lhs_hbm, w_hbm, res_hbm, gain_ref, *refs):
    refs = refs[n_after:]
    if with_norm:
        own_hbm, out_hbm = refs[:2]
        refs = refs[2:]
    else:
        out_hbm = refs[0]
        refs = refs[1:]
    lhs, w, part, in1, in2, res, own, norm, w_sem, l_sem, r_sem, o_sem, s1, r1, s2, r2, s3, r3, s4, r4 = refs
    n_w, depth, n_cols = w.shape
    cols = n_w * n_cols
    half = cols // 2
    rows = part.shape[2]
    block = rows * N_SUB
    me = lax.axis_index("tp")
    right, left = lax.rem(me + 1, n_tp), lax.rem(me + n_tp - 1, n_tp)
    far = lax.rem(me + 2, n_tp)
    sides = (right, left)
    lo, hi = pl.ds(0, half), pl.ds(half, half)
    halves = (lo, hi)

    def w_copy(d):
        return pltpu.make_async_copy(w_hbm.at[d], w.at[d], w_sem.at[d])

    def rows_of(b, s):
        return pl.ds(pl.multiple_of(b * block + s * rows, rows), rows)

    def lhs_copy(s, b):
        at = pl.ds(pl.multiple_of(s * rows, rows), rows)
        return pltpu.make_async_copy(lhs_hbm.at[rows_of(b, s), :], lhs.at[b, at, :], l_sem.at[s, b])

    for b in range(n_tp):
        lhs_copy(0, b).start()
    for d in range(n_w):
        w_copy(d).start()

    def load(s, carry):
        for b in range(n_tp):
            lhs_copy(s, b).start()
        return carry

    lax.fori_loop(1, N_SUB, load, 0)
    my_rows = pl.ds(pl.multiple_of(me * block, block), block)
    if with_norm:
        res_copies = [pltpu.make_async_copy(res_hbm.at[my_rows, :], res, r_sem.at[0])]
    else:
        wide = res_hbm.shape[1] // n_w
        res_copies = [pltpu.make_async_copy(res_hbm.at[:, pl.ds(d * wide + col_off, n_cols)], res.at[:, pl.ds(d * n_cols, n_cols)], r_sem.at[d]) for d in range(n_w)]
    for c in res_copies:
        c.start()

    barrier = pltpu.get_barrier_semaphore()
    for dev in sides:
        pl.semaphore_signal(barrier, inc=1, device_id={"tp": dev}, device_id_type=MESH)
    pl.semaphore_wait(barrier, 2)

    def remote(src, dst, send, recv, dev):
        return pltpu.make_async_remote_copy(src_ref=src, dst_ref=dst, send_sem=send, recv_sem=recv, device_id={"tp": dev}, device_id_type=MESH)

    def hop1(s, i):
        return remote(part.at[s, far, :, halves[i]], in1.at[s, i], s1.at[s, i], r1.at[s, i], sides[i])

    def hop2(s, i):
        return remote(part.at[s, sides[i]], in2.at[s, i], s2.at[s, i], r2.at[s, i], sides[i])

    def hop3(s, i):
        return remote(norm.at[s], out_hbm.at[rows_of(me, s), :], s3.at[s, i], r3.at[s, i], sides[i])

    def hop4(s, i):
        block_rows = rows_of(sides[1 - i], s)
        where = out_hbm.at[block_rows, halves[i]]
        return remote(where, where, s4.at[s, i], r4.at[s, i], sides[i])

    def stage_a(s):
        at = pl.ds(pl.multiple_of(s * rows, rows), rows)
        for b in range(n_tp):
            lhs_copy(s, b).wait()

        def one(d, carry):
            @pl.when(s == 0)
            def _():
                w_copy(d).wait()

            left_rows = lhs[:, at, :].reshape(n_tp * rows, depth)
            prod = jnp.dot(left_rows, w[d], preferred_element_type=F32).astype(BF16)
            part[s, :, :, pl.ds(pl.multiple_of(d * n_cols, n_cols), n_cols)] = prod.reshape(n_tp, rows, n_cols)
            for i in range(2):
                @pl.when(d == (i + 1) * (n_w // 2) - 1)
                def _():
                    hop1(s, i).start()
            return carry

        lax.fori_loop(0, n_w, one, 0)

    def stage_b(s):
        for i in range(2):
            hop1(s, i).wait_recv()
            dest = sides[i]
            mine = part[s, dest, :, halves[i]].astype(F32)
            part[s, dest, :, halves[i]] = (mine + in1[s, i].astype(F32)).astype(BF16)
            hop2(s, i).start()

    def stage_c(s):
        for i in range(2):
            hop2(s, i).wait_recv()
        step = 16

        def one(k, carry):
            at = pl.ds(pl.multiple_of(k * step, step), step)
            total = part[s, me, at, :].astype(F32) + in2[s, 0, at, :].astype(F32) + in2[s, 1, at, :].astype(F32)
            total = total.astype(BF16).astype(F32)
            res_at = pl.ds(pl.multiple_of(s * rows + k * step, step), step)
            mid = (res[res_at, :].astype(F32) + total).astype(BF16)
            if with_norm:
                own[s, at, :] = mid
                mid = mid.astype(F32)
                mean_sq = jnp.mean(mid * mid, axis=-1, keepdims=True)
                mid = (mid * lax.rsqrt(mean_sq + NORM_EPS) * gain_ref[...]).astype(BF16)
            norm[s, at, :] = mid
            return carry

        lax.fori_loop(0, rows // step, one, 0)
        if not with_norm:
            for i in range(2):
                hop3(s, i).start()
        local(s).start()
        if with_norm:
            keep(s).start()

    def local(s):
        where = pl.ds(pl.multiple_of(s * rows, rows), rows) if with_norm else rows_of(me, s)
        return pltpu.make_async_copy(norm.at[s], out_hbm.at[where, :], o_sem.at[s, 0])

    def keep(s):
        return pltpu.make_async_copy(own.at[s], own_hbm.at[pl.ds(pl.multiple_of(s * rows, rows), rows), :], o_sem.at[s, 1])

    def arrive3(s, i):
        where = out_hbm.at[rows_of(sides[1 - i], s), :]
        return remote(norm.at[s], where, s3.at[s, i], r3.at[s, i], sides[i])

    def arrive4(s, i):
        where = out_hbm.at[rows_of(far, s), halves[i]]
        return remote(where, where, s4.at[s, i], r4.at[s, i], sides[i])

    def stage_d(s):
        for i in range(2):
            arrive3(s, i).wait_recv()
            hop4(s, i).start()

    def tick(t, carry):
        @pl.when(t < N_SUB)
        def _():
            stage_a(t)

        @pl.when((t >= 1) & (t < N_SUB + 1))
        def _():
            stage_b(t - 1)

        @pl.when(t == 1)
        def _():
            for c in res_copies:
                c.wait()

        @pl.when((t >= 2) & (t < N_SUB + 2))
        def _():
            stage_c(t - 2)

        if not with_norm:
            @pl.when(t >= 3)
            def _():
                stage_d(t - 3)

        return carry

    lax.fori_loop(0, N_SUB + (2 if with_norm else 3), tick, 0)

    def drain(s, carry):
        local(s).wait()
        if with_norm:
            keep(s).wait()
        for i in range(2):
            hop1(s, i).wait_send()
            hop2(s, i).wait_send()
            if not with_norm:
                hop3(s, i).wait_send()
                hop4(s, i).wait_send()
                arrive4(s, i).wait_recv()
        return carry

    lax.fori_loop(0, N_SUB, drain, 0)


def sum_over_tp(n_tp, lhs, w, res, gain, col_off, with_norm, collective_id, after=()):
    tokens, depth = lhs.shape
    n_w, _, n_cols = w.shape
    cols = n_w * n_cols
    block = tokens // n_tp
    rows = block // N_SUB
    out_shape = [jax.ShapeDtypeStruct((block, cols), BF16)] * 2 if with_norm else [jax.ShapeDtypeStruct((tokens, cols), BF16)]
    dma = pltpu.SemaphoreType.DMA
    small = (N_SUB, rows, cols) if with_norm else (1, 16, 128)
    scratch = [
        pltpu.VMEM((n_tp, block, depth), BF16),
        pltpu.VMEM((n_w, depth, n_cols), BF16),
        pltpu.VMEM((N_SUB, n_tp, rows, cols), BF16),
        pltpu.VMEM((N_SUB, 2, rows, cols // 2), BF16),
        pltpu.VMEM((N_SUB, 2, rows, cols), BF16),
        pltpu.VMEM((block, cols), BF16),
        pltpu.VMEM(small, BF16),
        pltpu.VMEM((N_SUB, rows, cols), BF16),
        dma((n_w,)), dma((N_SUB, n_tp)), dma((n_w,)), dma((N_SUB, 2)),
    ] + [dma((N_SUB, 2))] * 8
    return pl.pallas_call(
        functools.partial(sum_kernel, n_tp, col_off, with_norm, len(after)),
        out_shape=out_shape,
        in_specs=[ANY, ANY, ANY, pl.BlockSpec(memory_space=pltpu.VMEM)] + [ANY] * len(after),
        out_specs=[ANY] * len(out_shape),
        scratch_shapes=scratch,
        compiler_params=pltpu.CompilerParams(collective_id=collective_id, has_side_effects=True, vmem_limit_bytes=VMEM_BIG),
        cost_estimate=pl.CostEstimate(flops=2 * tokens * cols * 30000, bytes_accessed=2 * (tokens * depth + depth * cols + 2 * tokens * cols), transcendentals=0),
        name="sum_tp_%d" % collective_id,
    )(lhs, w, res, gain, *after)


def gate_kernel(n_tp, own_hbm, w_hbm, all_hbm, gate_hbm, w, xs, ys, w_sem, x_sem, y_sem, l_sem, s1, r1, s2, r2):
    block, depth = own_hbm.shape
    part = block // 2
    half = depth // 2
    cols = w.shape[1]
    n_chunks = w_sem.shape[0]
    chunk = cols // n_chunks
    me = lax.axis_index("tp")
    right, left = lax.rem(me + 1, n_tp), lax.rem(me + n_tp - 1, n_tp)
    far = lax.rem(me + 2, n_tp)
    sides = (right, left)
    halves = (pl.ds(0, half), pl.ds(half, half))

    def rows_of(b, p):
        return pl.ds(pl.multiple_of(b * block + p * part, part), part)

    def part_of(p):
        return pl.ds(pl.multiple_of(p * part, part), part)

    def w_copy(n):
        at = pl.ds(pl.multiple_of(n * chunk, chunk), chunk)
        return pltpu.make_async_copy(w_hbm.at[:, at], w.at[:, at], w_sem.at[n])

    def remote(src, dst, send, recv, dev):
        return pltpu.make_async_remote_copy(src_ref=src, dst_ref=dst, send_sem=send, recv_sem=recv, device_id={"tp": dev}, device_id_type=MESH)

    def hop1(p, i):
        return remote(own_hbm.at[part_of(p), :], all_hbm.at[rows_of(me, p), :], s1.at[p, i], r1.at[p, i], sides[i])

    def hop2(p, i):
        where = all_hbm.at[rows_of(sides[1 - i], p), halves[i]]
        return remote(where, where, s2.at[p, i], r2.at[p, i], sides[i])

    def arrive1(p, i):
        where = all_hbm.at[rows_of(sides[1 - i], p), :]
        return remote(own_hbm.at[part_of(p), :], where, s1.at[p, i], r1.at[p, i], sides[i])

    def arrive2(p, i):
        where = all_hbm.at[rows_of(far, p), halves[i]]
        return remote(where, where, s2.at[p, i], r2.at[p, i], sides[i])

    def y_copy(k, rows):
        return pltpu.make_async_copy(ys.at[part_of(k)], gate_hbm.at[rows, :], y_sem.at[k])

    barrier = pltpu.get_barrier_semaphore()
    for dev in sides:
        pl.semaphore_signal(barrier, inc=1, device_id={"tp": dev}, device_id_type=MESH)
    pl.semaphore_wait(barrier, 2)
    for p in range(2):
        for i in range(2):
            hop1(p, i).start()
    own_copies = [pltpu.make_async_copy(own_hbm.at[part_of(p), :], xs.at[part_of(p)], x_sem.at[p]) for p in range(2)]
    for c in own_copies:
        c.start()
    for n in range(n_chunks):
        w_copy(n).start()
    for c in own_copies:
        c.wait()
    local_copies = [pltpu.make_async_copy(xs.at[part_of(p)], all_hbm.at[rows_of(me, p), :], l_sem.at[p]) for p in range(2)]
    for c in local_copies:
        c.start()

    def unit(u, carry):
        p = jnp.maximum(u - 1, 0)
        where = [rows_of(jnp.where(u == 0, me, sides[1 - k]), jnp.where(u == 0, k, p)) for k in range(2)]

        @pl.when(u >= 1)
        def _():
            for i in range(2):
                arrive1(p, i).wait_recv()
                hop2(p, i).start()

            @pl.when(u == 1)
            def _():
                for c in local_copies:
                    c.wait()

            loads = [pltpu.make_async_copy(all_hbm.at[where[k], :], xs.at[part_of(k)], x_sem.at[k]) for k in range(2)]
            for c in loads:
                c.start()
            for k in range(2):
                y_copy(k, where[k]).wait()
            for c in loads:
                c.wait()

        def one(n, c):
            at = pl.ds(pl.multiple_of(n * chunk, chunk), chunk)

            @pl.when(u == 0)
            def _():
                w_copy(n).wait()

            ys[:, at] = jnp.dot(xs[...], w[:, at], preferred_element_type=F32)
            return c

        lax.fori_loop(0, n_chunks, one, 0)
        for k in range(2):
            y_copy(k, where[k]).start()
        return carry

    lax.fori_loop(0, 3, unit, 0)
    y_copy(0, rows_of(far, 0)).wait()
    y_copy(1, rows_of(far, 1)).wait()

    def last(p, carry):
        for i in range(2):
            arrive2(p, i).wait_recv()
        load = pltpu.make_async_copy(all_hbm.at[rows_of(far, p), :], xs.at[part_of(p)], x_sem.at[p])
        load.start()
        load.wait()

        def one(n, c):
            at = pl.ds(pl.multiple_of(n * chunk, chunk), chunk)
            ys[part_of(p), at] = jnp.dot(xs[part_of(p), :], w[:, at], preferred_element_type=F32)
            return c

        lax.fori_loop(0, n_chunks, one, 0)
        y_copy(p, rows_of(far, p)).start()
        return carry

    lax.fori_loop(0, 2, last, 0)
    for p in range(2):
        y_copy(p, rows_of(far, p)).wait()
        for i in range(2):
            hop1(p, i).wait_send()
            hop2(p, i).wait_send()


def gather_and_gate(n_tp, own, w, collective_id):
    block, depth = own.shape
    cols = w.shape[1]
    tokens = n_tp * block
    chunk = next(c for c in (512, 256, 128) if cols % c == 0)
    dma = pltpu.SemaphoreType.DMA
    return pl.pallas_call(
        functools.partial(gate_kernel, n_tp),
        out_shape=[jax.ShapeDtypeStruct((tokens, depth), BF16), jax.ShapeDtypeStruct((tokens, cols), F32)],
        in_specs=[ANY, ANY],
        out_specs=[ANY, ANY],
        scratch_shapes=[
            pltpu.VMEM((depth, cols), BF16), pltpu.VMEM((block, depth), BF16), pltpu.VMEM((block, cols), F32),
            dma((cols // chunk,)), dma((2,)), dma((2,)), dma((2,)),
        ] + [dma((2, 2))] * 4,
        compiler_params=pltpu.CompilerParams(collective_id=collective_id, has_side_effects=True, vmem_limit_bytes=VMEM_BIG),
        cost_estimate=pl.CostEstimate(flops=2 * tokens * cols * depth * 3, bytes_accessed=2 * (tokens * depth + depth * cols + 2 * tokens * cols), transcendentals=0),
        name="gather_gate",
    )(own, w)


def join_kernel(n_w, a_ref, b_ref, o_ref):
    wa, wb = a_ref.shape[1] // n_w, b_ref.shape[1] // n_w
    for d in range(n_w):
        base = d * (wa + wb)
        o_ref[:, base:base + wa] = a_ref[:, d * wa:(d + 1) * wa]
        o_ref[:, base + wa:base + wa + wb] = b_ref[:, d * wb:(d + 1) * wb]


def join_columns(a, b, n_w):
    tokens = a.shape[0]
    rows = min(128, tokens)
    cols = a.shape[1] + b.shape[1]
    return pl.pallas_call(
        functools.partial(join_kernel, n_w),
        grid=(tokens // rows,),
        out_shape=jax.ShapeDtypeStruct((tokens, cols), BF16),
        in_specs=[pl.BlockSpec((rows, a.shape[1]), lambda i: (i, 0)), pl.BlockSpec((rows, b.shape[1]), lambda i: (i, 0))],
        out_specs=pl.BlockSpec((rows, cols), lambda i: (i, 0)),
        cost_estimate=pl.CostEstimate(flops=tokens * cols, bytes_accessed=4 * tokens * cols, transcendentals=0),
        name="join",
    )(a, b)


def solution(mesh):
    seq_spec = P(('dp', 'fsdp'), 'cp', None)
    pos_spec = P(('dp', 'fsdp'), 'cp')
    in_spec = P(GROUP_AXES, 'tp', None)
    out_spec = P('tp', None, GROUP_AXES)
    col_spec = P(GROUP_AXES, 'tp')
    row_spec = P('tp', GROUP_AXES)
    rep_spec = P(None)
    n_tp = mesh.shape['tp']
    n_w = mesh.shape['fsdp'] * mesh.shape['cp']

    def layer_local(hidden, positions, attn_gain, w_query, w_key, w_value, w_out, mlp_gain, w_gate, w_up, w_down):
        tokens, d_model = hidden.shape[1:]
        share, heads, head_dim = w_query.shape
        kv_heads = w_key.shape[1]
        w_qkv = jnp.concatenate([w.reshape(share, -1) for w in (w_query, w_key, w_value)], axis=1)
        full_qkv = lax.all_gather(w_qkv, GROUP_AXES, axis=0, tiled=True)
        full_out = lax.all_gather(w_out.reshape(heads * head_dim, share), GROUP_AXES, axis=0, tiled=False)
        full_gate = lax.all_gather(w_gate, GROUP_AXES, axis=0, tiled=True)
        full_up = lax.all_gather(w_up, GROUP_AXES, axis=0, tiled=True)
        cut = (share * 2 // 5) // 128 * 128
        x = hidden[0]
        normed = rms_norm(x.astype(F32), attn_gain)
        down0, down1, normed = lax.optimization_barrier((w_down[:, :cut], w_down[:, cut:], normed))
        full_down0 = lax.all_gather(down0, GROUP_AXES, axis=0, tiled=False)
        full_down1 = lax.all_gather(down1, GROUP_AXES, axis=0, tiled=False)
        cos, sin = rope_tables(positions[0], head_dim)
        qkv = project_qkv(normed, full_qkv, cos, sin, heads + kv_heads)
        kv = qkv[:, heads * head_dim:]
        kv_peer = lax.ppermute(kv, 'cp', [(0, 1), (1, 0)])
        c = lax.axis_index('cp')
        table = jnp.where(c == 0, jnp.array([0, 2, 3, 1, 0, 3], jnp.int32), jnp.array([2, 0, 1, 3, 1, 2], jnp.int32))
        kv_all = jnp.concatenate([kv, kv_peer], axis=0)
        k_all, vt_all = kv_all[:, :kv_heads * head_dim], kv_all[:, kv_heads * head_dim:].T
        mixed = attention(qkv, k_all, vt_all, table, heads, kv_heads, head_dim)
        mid_own, normed_own = sum_over_tp(n_tp, mixed, full_out, x, attn_gain_row(mlp_gain), 0, True, 0)
        normed_mlp, gate_proj = gather_and_gate(n_tp, normed_own, full_gate, 3)
        up_proj = jnp.dot(normed_mlp, full_up, preferred_element_type=F32)
        act = (jax.nn.silu(gate_proj) * up_proj).astype(BF16)
        piece0, = sum_over_tp(n_tp, act, full_down0, mid_own, attn_gain_row(mlp_gain), 0, False, 1)
        piece1, = sum_over_tp(n_tp, act, full_down1, mid_own, attn_gain_row(mlp_gain), cut, False, 2, after=(piece0,))
        return join_columns(piece0, piece1, n_w)[None]

    return jax.shard_map(layer_local, mesh=mesh, in_specs=(seq_spec, pos_spec, rep_spec, in_spec, in_spec, in_spec, out_spec, rep_spec, col_spec, col_spec, row_spec), out_specs=seq_spec, check_vma=False)


def attn_gain_row(gain):
    return gain[None, :]
```

```python
import functools

import jax
import jax.numpy as jnp
from jax import lax
from jax.experimental import pallas as pl
from jax.experimental.pallas import tpu as pltpu
from jax.sharding import PartitionSpec as P

ROPE_THETA = 500000.0
NORM_EPS = 1e-5
GROUP_AXES = ('fsdp', 'cp')
N_SUB = 12
F32 = jnp.float32
BF16 = jnp.bfloat16
MESH = pl.DeviceIdType.MESH
VMEM_BIG = 58 * 1024 * 1024
ANY = pl.BlockSpec(memory_space=pl.ANY)


def rms_norm(hidden_f32, gain):
    mean_sq = jnp.mean(hidden_f32 * hidden_f32, axis=-1, keepdims=True)
    return (hidden_f32 * lax.rsqrt(mean_sq + NORM_EPS) * gain).astype(BF16)


def rope_tables(positions, head_dim):
    inv_freq = ROPE_THETA ** (-jnp.arange(0, head_dim, 2, dtype=F32) / head_dim)
    angles = positions.astype(F32)[..., None] * inv_freq
    cos, sin = jnp.cos(angles), jnp.sin(angles)
    return jnp.concatenate([cos, cos], axis=-1), jnp.concatenate([-sin, sin], axis=-1)


def qkv_kernel(head_dim, rope_heads, a_ref, w_ref, cos_ref, sin_ref, o_ref):
    cols = w_ref.shape[1]
    step = 4 * head_dim
    cos, sin = cos_ref[...], sin_ref[...]
    for start in range(0, cols, step):
        proj = jnp.dot(a_ref[...], w_ref[:, start:start + step], preferred_element_type=F32)
        for k in range(step // head_dim):
            x = proj[:, k * head_dim:(k + 1) * head_dim]
            if start // head_dim + k < rope_heads:
                x = x * cos + pltpu.roll(x, head_dim // 2, 1) * sin
            o_ref[:, start + k * head_dim:start + (k + 1) * head_dim] = x.astype(BF16)


def project_qkv(a, w, cos, sin, rope_heads):
    tokens, d_model = a.shape
    cols, head_dim = w.shape[1], cos.shape[1]
    rows = min(256, tokens)
    return pl.pallas_call(
        functools.partial(qkv_kernel, head_dim, rope_heads),
        grid=(tokens // rows,),
        out_shape=jax.ShapeDtypeStruct((tokens, cols), BF16),
        in_specs=[
            pl.BlockSpec((rows, d_model), lambda i: (i, 0)),
            pl.BlockSpec((d_model, cols), lambda i: (0, 0), pipeline_mode=pl.Buffered(1)),
            pl.BlockSpec((rows, head_dim), lambda i: (i, 0)),
            pl.BlockSpec((rows, head_dim), lambda i: (i, 0)),
        ],
        out_specs=pl.BlockSpec((rows, cols), lambda i: (i, 0)),
        compiler_params=pltpu.CompilerParams(vmem_limit_bytes=VMEM_BIG),
        cost_estimate=pl.CostEstimate(flops=2 * tokens * d_model * cols, bytes_accessed=2 * (tokens * d_model + d_model * cols + tokens * cols), transcendentals=0),
        name="qkv",
    )(a, w, cos, sin)


def attn_kernel(group, head_dim, per_seg, table_ref, q_ref, k_ref, vt_ref, o_ref, m_sc, l_sc, acc_sc):
    blk = q_ref.shape[0]
    seg_rows = per_seg * blk
    qi = pl.program_id(1)
    true_seg = table_ref[4 + qi // per_seg]
    scale = (head_dim ** -0.5) * 1.4426950408889634
    m_sc[...] = jnp.full(m_sc.shape, -1e30, F32)
    l_sc[...] = jnp.zeros(l_sc.shape, F32)
    acc_sc[...] = jnp.zeros(acc_sc.shape, F32)

    def step(j, n_keys, within):
        rows = pl.ds(pl.multiple_of(table_ref[j] * seg_rows, seg_rows), n_keys)
        k, vt = k_ref[rows, :], vt_ref[:, rows]
        for h in range(group):
            q = q_ref[:, h * head_dim:(h + 1) * head_dim]
            s = lax.dot_general(k, q, (((1,), (1,)), ((), ())), preferred_element_type=F32) * scale
            if within is not None:
                keep = lax.broadcasted_iota(jnp.int32, s.shape, 0) <= lax.broadcasted_iota(jnp.int32, s.shape, 1) + within
                s = jnp.where(keep, s, -1e30)
            m_old = m_sc[h]
            m_new = jnp.maximum(m_old, jnp.max(s, axis=0, keepdims=True))
            alpha = jnp.exp2(m_old - m_new)
            p = jnp.exp2(s - m_new)
            l_sc[h] = l_sc[h] * alpha + jnp.sum(p, axis=0, keepdims=True)
            acc_sc[h] = acc_sc[h] * alpha + jnp.dot(vt, p.astype(BF16), preferred_element_type=F32)
            m_sc[h] = m_new

    def body(j, carry):
        step(j, seg_rows, None)
        return carry

    lax.fori_loop(0, true_seg, body, 0)
    for w in range(per_seg):
        @pl.when(lax.rem(qi, per_seg) == w)
        def _():
            step(true_seg, (w + 1) * blk, w * blk)

    for h in range(group):
        o_ref[:, h * head_dim:(h + 1) * head_dim] = (acc_sc[h] / l_sc[h]).T.astype(BF16)


def attention(qkv, k_all, vt_all, table, heads, kv_heads, head_dim):
    tokens, keys = qkv.shape[0], k_all.shape[0]
    seg_rows = tokens // 2
    blk = min(256, seg_rows)
    per_seg = seg_rows // blk
    group = heads // kv_heads
    return pl.pallas_call(
        functools.partial(attn_kernel, group, head_dim, per_seg),
        grid_spec=pltpu.PrefetchScalarGridSpec(
            num_scalar_prefetch=1,
            grid=(kv_heads, tokens // blk),
            in_specs=[
                pl.BlockSpec((blk, group * head_dim), lambda g, i, t: (i, g)),
                pl.BlockSpec((keys, head_dim), lambda g, i, t: (0, g)),
                pl.BlockSpec((head_dim, keys), lambda g, i, t: (g, 0)),
            ],
            out_specs=pl.BlockSpec((blk, group * head_dim), lambda g, i, t: (i, g)),
            scratch_shapes=[pltpu.VMEM((group, 1, blk), F32), pltpu.VMEM((group, 1, blk), F32), pltpu.VMEM((group, head_dim, blk), F32)],
        ),
        out_shape=jax.ShapeDtypeStruct((tokens, heads * head_dim), BF16),
        compiler_params=pltpu.CompilerParams(vmem_limit_bytes=32 * 1024 * 1024),
        cost_estimate=pl.CostEstimate(flops=2 * tokens * keys * heads * head_dim * 2, bytes_accessed=2 * (2 * tokens * heads * head_dim + 4 * keys * head_dim), transcendentals=tokens * keys * heads),
        name="attn",
    )(table, qkv, k_all, vt_all)


def sum_kernel(n_tp, col_off, with_norm, n_after, lhs_hbm, w_hbm, res_hbm, gain_ref, *refs):
    refs = refs[n_after:]
    if with_norm:
        own_hbm, out_hbm = refs[:2]
        refs = refs[2:]
    else:
        out_hbm = refs[0]
        refs = refs[1:]
    lhs, w, part, in1, in2, res, own, norm, w_sem, l_sem, r_sem, o_sem, s1, r1, s2, r2, s3, r3, s4, r4 = refs
    n_w, depth, n_cols = w.shape
    cols = n_w * n_cols
    half = cols // 2
    rows = part.shape[2]
    block = rows * N_SUB
    me = lax.axis_index("tp")
    right, left = lax.rem(me + 1, n_tp), lax.rem(me + n_tp - 1, n_tp)
    far = lax.rem(me + 2, n_tp)
    sides = (right, left)
    lo, hi = pl.ds(0, half), pl.ds(half, half)
    halves = (lo, hi)

    def w_copy(d):
        return pltpu.make_async_copy(w_hbm.at[d], w.at[d], w_sem.at[d])

    def rows_of(b, s):
        return pl.ds(pl.multiple_of(b * block + s * rows, rows), rows)

    def lhs_copy(s, b):
        at = pl.ds(pl.multiple_of(s * rows, rows), rows)
        return pltpu.make_async_copy(lhs_hbm.at[rows_of(b, s), :], lhs.at[b, at, :], l_sem.at[s, b])

    for b in range(n_tp):
        lhs_copy(0, b).start()
    for d in range(n_w):
        w_copy(d).start()

    def load(s, carry):
        for b in range(n_tp):
            lhs_copy(s, b).start()
        return carry

    lax.fori_loop(1, N_SUB, load, 0)
    my_rows = pl.ds(pl.multiple_of(me * block, block), block)
    if with_norm:
        res_copies = [pltpu.make_async_copy(res_hbm.at[my_rows, :], res, r_sem.at[0])]
    else:
        wide = res_hbm.shape[1] // n_w
        res_copies = [pltpu.make_async_copy(res_hbm.at[:, pl.ds(d * wide + col_off, n_cols)], res.at[:, pl.ds(d * n_cols, n_cols)], r_sem.at[d]) for d in range(n_w)]
    for c in res_copies:
        c.start()

    barrier = pltpu.get_barrier_semaphore()
    for dev in sides:
        pl.semaphore_signal(barrier, inc=1, device_id={"tp": dev}, device_id_type=MESH)
    pl.semaphore_wait(barrier, 2)

    def remote(src, dst, send, recv, dev):
        return pltpu.make_async_remote_copy(src_ref=src, dst_ref=dst, send_sem=send, recv_sem=recv, device_id={"tp": dev}, device_id_type=MESH)

    def hop1(s, i):
        return remote(part.at[s, far, :, halves[i]], in1.at[s, i], s1.at[s, i], r1.at[s, i], sides[i])

    def hop2(s, i):
        return remote(part.at[s, sides[i]], in2.at[s, i], s2.at[s, i], r2.at[s, i], sides[i])

    def hop3(s, i):
        return remote(norm.at[s], out_hbm.at[rows_of(me, s), :], s3.at[s, i], r3.at[s, i], sides[i])

    def hop4(s, i):
        block_rows = rows_of(sides[1 - i], s)
        where = out_hbm.at[block_rows, halves[i]]
        return remote(where, where, s4.at[s, i], r4.at[s, i], sides[i])

    def stage_a(s):
        at = pl.ds(pl.multiple_of(s * rows, rows), rows)
        for b in range(n_tp):
            lhs_copy(s, b).wait()

        def one(d, carry):
            @pl.when(s == 0)
            def _():
                w_copy(d).wait()

            left_rows = lhs[:, at, :].reshape(n_tp * rows, depth)
            prod = jnp.dot(left_rows, w[d], preferred_element_type=F32).astype(BF16)
            part[s, :, :, pl.ds(pl.multiple_of(d * n_cols, n_cols), n_cols)] = prod.reshape(n_tp, rows, n_cols)
            for i in range(2):
                @pl.when(d == (i + 1) * (n_w // 2) - 1)
                def _():
                    hop1(s, i).start()
            return carry

        lax.fori_loop(0, n_w, one, 0)

    def stage_b(s):
        for i in range(2):
            hop1(s, i).wait_recv()
            dest = sides[i]
            mine = part[s, dest, :, halves[i]].astype(F32)
            part[s, dest, :, halves[i]] = (mine + in1[s, i].astype(F32)).astype(BF16)
            hop2(s, i).start()

    def stage_c(s):
        for i in range(2):
            hop2(s, i).wait_recv()
        step = 16

        def one(k, carry):
            at = pl.ds(pl.multiple_of(k * step, step), step)
            total = part[s, me, at, :].astype(F32) + in2[s, 0, at, :].astype(F32) + in2[s, 1, at, :].astype(F32)
            total = total.astype(BF16).astype(F32)
            res_at = pl.ds(pl.multiple_of(s * rows + k * step, step), step)
            mid = (res[res_at, :].astype(F32) + total).astype(BF16)
            if with_norm:
                own[s, at, :] = mid
                mid = mid.astype(F32)
                mean_sq = jnp.mean(mid * mid, axis=-1, keepdims=True)
                mid = (mid * lax.rsqrt(mean_sq + NORM_EPS) * gain_ref[...]).astype(BF16)
            norm[s, at, :] = mid
            return carry

        lax.fori_loop(0, rows // step, one, 0)
        if not with_norm:
            for i in range(2):
                hop3(s, i).start()
        local(s).start()
        if with_norm:
            keep(s).start()

    def local(s):
        where = pl.ds(pl.multiple_of(s * rows, rows), rows) if with_norm else rows_of(me, s)
        return pltpu.make_async_copy(norm.at[s], out_hbm.at[where, :], o_sem.at[s, 0])

    def keep(s):
        return pltpu.make_async_copy(own.at[s], own_hbm.at[pl.ds(pl.multiple_of(s * rows, rows), rows), :], o_sem.at[s, 1])

    def arrive3(s, i):
        where = out_hbm.at[rows_of(sides[1 - i], s), :]
        return remote(norm.at[s], where, s3.at[s, i], r3.at[s, i], sides[i])

    def arrive4(s, i):
        where = out_hbm.at[rows_of(far, s), halves[i]]
        return remote(where, where, s4.at[s, i], r4.at[s, i], sides[i])

    def stage_d(s):
        for i in range(2):
            arrive3(s, i).wait_recv()
            hop4(s, i).start()

    def tick(t, carry):
        @pl.when(t < N_SUB)
        def _():
            stage_a(t)

        @pl.when((t >= 1) & (t < N_SUB + 1))
        def _():
            stage_b(t - 1)

        @pl.when(t == 1)
        def _():
            for c in res_copies:
                c.wait()

        @pl.when((t >= 2) & (t < N_SUB + 2))
        def _():
            stage_c(t - 2)

        if not with_norm:
            @pl.when(t >= 3)
            def _():
                stage_d(t - 3)

        return carry

    lax.fori_loop(0, N_SUB + (2 if with_norm else 3), tick, 0)

    def drain(s, carry):
        local(s).wait()
        if with_norm:
            keep(s).wait()
        for i in range(2):
            hop1(s, i).wait_send()
            hop2(s, i).wait_send()
            if not with_norm:
                hop3(s, i).wait_send()
                hop4(s, i).wait_send()
                arrive4(s, i).wait_recv()
        return carry

    lax.fori_loop(0, N_SUB, drain, 0)


def sum_over_tp(n_tp, lhs, w, res, gain, col_off, with_norm, collective_id, after=()):
    tokens, depth = lhs.shape
    n_w, _, n_cols = w.shape
    cols = n_w * n_cols
    block = tokens // n_tp
    rows = block // N_SUB
    out_shape = [jax.ShapeDtypeStruct((block, cols), BF16)] * 2 if with_norm else [jax.ShapeDtypeStruct((tokens, cols), BF16)]
    dma = pltpu.SemaphoreType.DMA
    small = (N_SUB, rows, cols) if with_norm else (1, 16, 128)
    scratch = [
        pltpu.VMEM((n_tp, block, depth), BF16),
        pltpu.VMEM((n_w, depth, n_cols), BF16),
        pltpu.VMEM((N_SUB, n_tp, rows, cols), BF16),
        pltpu.VMEM((N_SUB, 2, rows, cols // 2), BF16),
        pltpu.VMEM((N_SUB, 2, rows, cols), BF16),
        pltpu.VMEM((block, cols), BF16),
        pltpu.VMEM(small, BF16),
        pltpu.VMEM((N_SUB, rows, cols), BF16),
        dma((n_w,)), dma((N_SUB, n_tp)), dma((n_w,)), dma((N_SUB, 2)),
    ] + [dma((N_SUB, 2))] * 8
    return pl.pallas_call(
        functools.partial(sum_kernel, n_tp, col_off, with_norm, len(after)),
        out_shape=out_shape,
        in_specs=[ANY, ANY, ANY, pl.BlockSpec(memory_space=pltpu.VMEM)] + [ANY] * len(after),
        out_specs=[ANY] * len(out_shape),
        scratch_shapes=scratch,
        compiler_params=pltpu.CompilerParams(collective_id=collective_id, has_side_effects=True, vmem_limit_bytes=VMEM_BIG),
        cost_estimate=pl.CostEstimate(flops=2 * tokens * cols * 30000, bytes_accessed=2 * (tokens * depth + depth * cols + 2 * tokens * cols), transcendentals=0),
        name="sum_tp_%d" % collective_id,
    )(lhs, w, res, gain, *after)


def gate_kernel(n_tp, own_hbm, w_hbm, all_hbm, gate_hbm, w, xs, ys, w_sem, x_sem, y_sem, l_sem, s1, r1, s2, r2):
    block, depth = own_hbm.shape
    part = block // 2
    half = depth // 2
    cols = w.shape[1]
    n_chunks = w_sem.shape[0]
    chunk = cols // n_chunks
    me = lax.axis_index("tp")
    right, left = lax.rem(me + 1, n_tp), lax.rem(me + n_tp - 1, n_tp)
    far = lax.rem(me + 2, n_tp)
    sides = (right, left)
    halves = (pl.ds(0, half), pl.ds(half, half))

    def rows_of(b, p):
        return pl.ds(pl.multiple_of(b * block + p * part, part), part)

    def part_of(p):
        return pl.ds(pl.multiple_of(p * part, part), part)

    def w_copy(n):
        at = pl.ds(pl.multiple_of(n * chunk, chunk), chunk)
        return pltpu.make_async_copy(w_hbm.at[:, at], w.at[:, at], w_sem.at[n])

    def remote(src, dst, send, recv, dev):
        return pltpu.make_async_remote_copy(src_ref=src, dst_ref=dst, send_sem=send, recv_sem=recv, device_id={"tp": dev}, device_id_type=MESH)

    def hop1(p, i):
        return remote(own_hbm.at[part_of(p), :], all_hbm.at[rows_of(me, p), :], s1.at[p, i], r1.at[p, i], sides[i])

    def hop2(p, i):
        where = all_hbm.at[rows_of(sides[1 - i], p), halves[i]]
        return remote(where, where, s2.at[p, i], r2.at[p, i], sides[i])

    def arrive1(p, i):
        where = all_hbm.at[rows_of(sides[1 - i], p), :]
        return remote(own_hbm.at[part_of(p), :], where, s1.at[p, i], r1.at[p, i], sides[i])

    def arrive2(p, i):
        where = all_hbm.at[rows_of(far, p), halves[i]]
        return remote(where, where, s2.at[p, i], r2.at[p, i], sides[i])

    def y_copy(k, rows):
        return pltpu.make_async_copy(ys.at[part_of(k)], gate_hbm.at[rows, :], y_sem.at[k])

    barrier = pltpu.get_barrier_semaphore()
    for dev in sides:
        pl.semaphore_signal(barrier, inc=1, device_id={"tp": dev}, device_id_type=MESH)
    pl.semaphore_wait(barrier, 2)
    for p in range(2):
        for i in range(2):
            hop1(p, i).start()
    own_copies = [pltpu.make_async_copy(own_hbm.at[part_of(p), :], xs.at[part_of(p)], x_sem.at[p]) for p in range(2)]
    for c in own_copies:
        c.start()
    for n in range(n_chunks):
        w_copy(n).start()
    for c in own_copies:
        c.wait()
    local_copies = [pltpu.make_async_copy(xs.at[part_of(p)], all_hbm.at[rows_of(me, p), :], l_sem.at[p]) for p in range(2)]
    for c in local_copies:
        c.start()

    def unit(u, carry):
        p = jnp.maximum(u - 1, 0)
        where = [rows_of(jnp.where(u == 0, me, sides[1 - k]), jnp.where(u == 0, k, p)) for k in range(2)]

        @pl.when(u >= 1)
        def _():
            for i in range(2):
                arrive1(p, i).wait_recv()
                hop2(p, i).start()

            @pl.when(u == 1)
            def _():
                for c in local_copies:
                    c.wait()

            loads = [pltpu.make_async_copy(all_hbm.at[where[k], :], xs.at[part_of(k)], x_sem.at[k]) for k in range(2)]
            for c in loads:
                c.start()
            for k in range(2):
                y_copy(k, where[k]).wait()
            for c in loads:
                c.wait()

        def one(n, c):
            at = pl.ds(pl.multiple_of(n * chunk, chunk), chunk)

            @pl.when(u == 0)
            def _():
                w_copy(n).wait()

            ys[:, at] = jnp.dot(xs[...], w[:, at], preferred_element_type=F32)
            return c

        lax.fori_loop(0, n_chunks, one, 0)
        for k in range(2):
            y_copy(k, where[k]).start()
        return carry

    lax.fori_loop(0, 3, unit, 0)
    y_copy(0, rows_of(far, 0)).wait()
    y_copy(1, rows_of(far, 1)).wait()

    def last(p, carry):
        for i in range(2):
            arrive2(p, i).wait_recv()
        load = pltpu.make_async_copy(all_hbm.at[rows_of(far, p), :], xs.at[part_of(p)], x_sem.at[p])
        load.start()
        load.wait()

        def one(n, c):
            at = pl.ds(pl.multiple_of(n * chunk, chunk), chunk)
            ys[part_of(p), at] = jnp.dot(xs[part_of(p), :], w[:, at], preferred_element_type=F32)
            return c

        lax.fori_loop(0, n_chunks, one, 0)
        y_copy(p, rows_of(far, p)).start()
        return carry

    lax.fori_loop(0, 2, last, 0)
    for p in range(2):
        y_copy(p, rows_of(far, p)).wait()
        for i in range(2):
            hop1(p, i).wait_send()
            hop2(p, i).wait_send()


def gather_and_gate(n_tp, own, w, collective_id):
    block, depth = own.shape
    cols = w.shape[1]
    tokens = n_tp * block
    chunk = next(c for c in (512, 256, 128) if cols % c == 0)
    dma = pltpu.SemaphoreType.DMA
    return pl.pallas_call(
        functools.partial(gate_kernel, n_tp),
        out_shape=[jax.ShapeDtypeStruct((tokens, depth), BF16), jax.ShapeDtypeStruct((tokens, cols), F32)],
        in_specs=[ANY, ANY],
        out_specs=[ANY, ANY],
        scratch_shapes=[
            pltpu.VMEM((depth, cols), BF16), pltpu.VMEM((block, depth), BF16), pltpu.VMEM((block, cols), F32),
            dma((cols // chunk,)), dma((2,)), dma((2,)), dma((2,)),
        ] + [dma((2, 2))] * 4,
        compiler_params=pltpu.CompilerParams(collective_id=collective_id, has_side_effects=True, vmem_limit_bytes=VMEM_BIG),
        cost_estimate=pl.CostEstimate(flops=2 * tokens * cols * depth * 3, bytes_accessed=2 * (tokens * depth + depth * cols + 2 * tokens * cols), transcendentals=0),
        name="gather_gate",
    )(own, w)


def join_kernel(n_w, a_ref, b_ref, o_ref):
    wa, wb = a_ref.shape[1] // n_w, b_ref.shape[1] // n_w
    for d in range(n_w):
        base = d * (wa + wb)
        o_ref[:, base:base + wa] = a_ref[:, d * wa:(d + 1) * wa]
        o_ref[:, base + wa:base + wa + wb] = b_ref[:, d * wb:(d + 1) * wb]


def join_columns(a, b, n_w):
    tokens = a.shape[0]
    rows = min(384, tokens)
    cols = a.shape[1] + b.shape[1]
    return pl.pallas_call(
        functools.partial(join_kernel, n_w),
        grid=(tokens // rows,),
        out_shape=jax.ShapeDtypeStruct((tokens, cols), BF16),
        in_specs=[pl.BlockSpec((rows, a.shape[1]), lambda i: (i, 0)), pl.BlockSpec((rows, b.shape[1]), lambda i: (i, 0))],
        out_specs=pl.BlockSpec((rows, cols), lambda i: (i, 0)),
        compiler_params=pltpu.CompilerParams(vmem_limit_bytes=VMEM_BIG),
        cost_estimate=pl.CostEstimate(flops=tokens * cols, bytes_accessed=4 * tokens * cols, transcendentals=0),
        name="join",
    )(a, b)


def solution(mesh):
    seq_spec = P(('dp', 'fsdp'), 'cp', None)
    pos_spec = P(('dp', 'fsdp'), 'cp')
    in_spec = P(GROUP_AXES, 'tp', None)
    out_spec = P('tp', None, GROUP_AXES)
    col_spec = P(GROUP_AXES, 'tp')
    row_spec = P('tp', GROUP_AXES)
    rep_spec = P(None)
    n_tp = mesh.shape['tp']
    n_w = mesh.shape['fsdp'] * mesh.shape['cp']

    def layer_local(hidden, positions, attn_gain, w_query, w_key, w_value, w_out, mlp_gain, w_gate, w_up, w_down):
        tokens, d_model = hidden.shape[1:]
        share, heads, head_dim = w_query.shape
        kv_heads = w_key.shape[1]
        w_qkv = jnp.concatenate([w.reshape(share, -1) for w in (w_query, w_key, w_value)], axis=1)
        full_qkv = lax.all_gather(w_qkv, GROUP_AXES, axis=0, tiled=True)
        full_out = lax.all_gather(w_out.reshape(heads * head_dim, share), GROUP_AXES, axis=0, tiled=False)
        full_gate = lax.all_gather(w_gate, GROUP_AXES, axis=0, tiled=True)
        full_up = lax.all_gather(w_up, GROUP_AXES, axis=0, tiled=True)
        cut = (share * 2 // 5) // 128 * 128
        x = hidden[0]
        normed = rms_norm(x.astype(F32), attn_gain)
        down0, down1, normed = lax.optimization_barrier((w_down[:, :cut], w_down[:, cut:], normed))
        full_down0 = lax.all_gather(down0, GROUP_AXES, axis=0, tiled=False)
        full_down1 = lax.all_gather(down1, GROUP_AXES, axis=0, tiled=False)
        cos, sin = rope_tables(positions[0], head_dim)
        qkv = project_qkv(normed, full_qkv, cos, sin, heads + kv_heads)
        kv = qkv[:, heads * head_dim:]
        kv_peer = lax.ppermute(kv, 'cp', [(0, 1), (1, 0)])
        c = lax.axis_index('cp')
        table = jnp.where(c == 0, jnp.array([0, 2, 3, 1, 0, 3], jnp.int32), jnp.array([2, 0, 1, 3, 1, 2], jnp.int32))
        kv_all = jnp.concatenate([kv, kv_peer], axis=0)
        k_all, vt_all = kv_all[:, :kv_heads * head_dim], kv_all[:, kv_heads * head_dim:].T
        mixed = attention(qkv, k_all, vt_all, table, heads, kv_heads, head_dim)
        mid_own, normed_own = sum_over_tp(n_tp, mixed, full_out, x, attn_gain_row(mlp_gain), 0, True, 0)
        normed_mlp, gate_proj = gather_and_gate(n_tp, normed_own, full_gate, 3)
        up_proj = jnp.dot(normed_mlp, full_up, preferred_element_type=F32)
        act = (jax.nn.silu(gate_proj) * up_proj).astype(BF16)
        piece0, = sum_over_tp(n_tp, act, full_down0, mid_own, attn_gain_row(mlp_gain), 0, False, 1)
        piece1, = sum_over_tp(n_tp, act, full_down1, mid_own, attn_gain_row(mlp_gain), cut, False, 2, after=(piece0,))
        return join_columns(piece0, piece1, n_w)[None]

    return jax.shard_map(layer_local, mesh=mesh, in_specs=(seq_spec, pos_spec, rep_spec, in_spec, in_spec, in_spec, out_spec, rep_spec, col_spec, col_spec, row_spec), out_specs=seq_spec, check_vma=False)


def attn_gain_row(gain):
    return gain[None, :]
```
